16 devices in a mesh: dp: 2 (over y, z), ep: 8 (over x, core).
Axes of the slice: x: 4, y: 2, z: 1, core: 2. Of those that a mesh axis runs over, the one named last changes fastest.
The devices are a block of a 4x4x8 slice.
Arguments:
- tokens: bfloat16 [4096, 1536], P(('dp', 'ep')), parts along dimension 0
- expert_ids: int32 [4096, 6], P(('dp', 'ep')), parts along dimension 0
- gate_vals: float32 [4096, 6], P(('dp', 'ep')), parts along dimension 0
- w_gate: bfloat16 [64, 1536, 512], P('ep')
- w_up: bfloat16 [64, 1536, 512], P('ep')
- w_down: bfloat16 [64, 512, 1536], P('ep')
Outputs:
- output: bfloat16 [4096, 1536], P(('dp', 'ep')), parts along dimension 0
There are 2 independent parts. The reference program is written for one: setup_inputs(seed, part) draws one part's arguments, and reference() takes and returns one part's arrays. A program takes and returns all parts, laid end to end along the dimension named above; an argument that names none is the same for every part.
All inputs are finite; a program needn't handle non-finite values.
Results may differ from the reference program's by a relative error of at most 0.00663984.
Values are sent between devices in bfloat16 or wider.
A program may use at most 768 MiB of HBM per device.

```python
import jax
import jax.numpy as jnp
from jax import lax

D_MODEL = 1536
FFN_DIM = 512
NUM_EXPERTS = 64
TOP_K = 6
GROUP = 8
TOK_DEV = 256

DEV_LIMIT = TOP_K // 2
LOCAL_EXPERTS = NUM_EXPERTS // GROUP
PAIR_CAP = TOK_DEV * DEV_LIMIT // GROUP
EXPERT_CAP = TOK_DEV * TOP_K * GROUP // NUM_EXPERTS
TOKENS = GROUP * TOK_DEV


def perm_rows(rand_key, row_count, perm_size):
    return jax.vmap(lambda sub_key: jax.random.permutation(sub_key, perm_size))(jax.random.split(rand_key, row_count))


def draw_routing(rand_key):
    key_src, key_dst, key_slot = jax.random.split(rand_key, 3)
    src_perm = perm_rows(key_src, GROUP, GROUP)
    dst_perm = perm_rows(key_dst, GROUP, LOCAL_EXPERTS)
    flat_pos = jnp.arange(TOK_DEV)[:, None] * DEV_LIMIT + jnp.arange(DEV_LIMIT)[None, :]
    dest_dev = src_perm[:, flat_pos % GROUP]
    recv_row = jnp.arange(GROUP)[:, None, None] * PAIR_CAP + (flat_pos // GROUP)[None, :, :]
    first_loc = dst_perm[dest_dev, (2 * recv_row) % LOCAL_EXPERTS]
    second_loc = dst_perm[dest_dev, (2 * recv_row + 1) % LOCAL_EXPERTS]
    pair_ids = jnp.stack([first_loc, second_loc], axis=-1) + dest_dev[..., None] * LOCAL_EXPERTS
    ordered = pair_ids.reshape(TOKENS, TOP_K)
    scores = jax.random.randint(key_slot, (TOKENS, TOP_K), 0, 1 << 20) * TOP_K + jnp.arange(TOP_K)[None, :]
    slot_order = jnp.argsort(scores, axis=1)
    return jnp.take_along_axis(ordered, slot_order, axis=1).astype(jnp.int32)


def setup_inputs(seed: int = 0, part: int = 0) -> dict:
    base_key = jax.random.key(seed)
    key_x, key_route, key_gate = jax.random.split(jax.random.fold_in(base_key, part), 3)
    key_wg, key_wu, key_wd = jax.random.split(jax.random.key(seed + 1), 3)
    in_scale = D_MODEL ** -0.5
    out_scale = 2.0 * FFN_DIM ** -0.5
    tokens = jax.random.normal(key_x, (TOKENS, D_MODEL), jnp.float32).astype(jnp.bfloat16)
    expert_ids = draw_routing(key_route)
    logits = 1.5 * jax.random.normal(key_gate, (TOKENS, TOP_K), jnp.float32)
    gate_vals = jax.nn.softmax(logits, axis=-1)
    w_gate = (in_scale * jax.random.normal(key_wg, (NUM_EXPERTS, D_MODEL, FFN_DIM), jnp.float32)).astype(jnp.bfloat16)
    w_up = (in_scale * jax.random.normal(key_wu, (NUM_EXPERTS, D_MODEL, FFN_DIM), jnp.float32)).astype(jnp.bfloat16)
    w_down = (out_scale * jax.random.normal(key_wd, (NUM_EXPERTS, FFN_DIM, D_MODEL), jnp.float32)).astype(jnp.bfloat16)
    return {'tokens': tokens, 'expert_ids': expert_ids, 'gate_vals': gate_vals, 'w_gate': w_gate, 'w_up': w_up, 'w_down': w_down}


def expert_ffn(row_in, gate_mat, up_mat, down_mat):
    gate_act = jnp.dot(row_in, gate_mat, preferred_element_type=jnp.float32)
    up_act = jnp.dot(row_in, up_mat, preferred_element_type=jnp.float32)
    hidden = (jax.nn.silu(gate_act) * up_act).astype(jnp.bfloat16)
    return jnp.dot(hidden, down_mat, preferred_element_type=jnp.float32).astype(jnp.bfloat16)


def reference(tokens, expert_ids, gate_vals, w_gate, w_up, w_down):
    pair_count = TOKENS * TOP_K
    flat_ids = expert_ids.reshape(pair_count)
    pair_index = jnp.arange(pair_count, dtype=jnp.int32)

    def one_expert(map_item):
        expert, gate_mat, up_mat, down_mat = map_item
        member = flat_ids == expert
        slot_pos = jnp.where(member, jnp.cumsum(member.astype(jnp.int32)) - 1, EXPERT_CAP)
        pair_list = jnp.full((EXPERT_CAP,), pair_count, jnp.int32).at[slot_pos].set(pair_index, mode='drop')
        row_in = tokens[jnp.minimum(pair_list, pair_count - 1) // TOP_K]
        return pair_list, expert_ffn(row_in, gate_mat, up_mat, down_mat)

    pair_lists, expert_rows = lax.map(one_expert, (jnp.arange(NUM_EXPERTS, dtype=jnp.int32), w_gate, w_up, w_down))
    pair_out = jnp.zeros((pair_count, D_MODEL), jnp.bfloat16).at[pair_lists.reshape(-1)].set(expert_rows.reshape(-1, D_MODEL), mode='drop')
    earlier = jnp.arange(TOP_K)[None, :] < jnp.arange(TOP_K)[:, None]

    def combine_block(blk_item):
        rows_in, ids_in, gate_in, outs_in = blk_item
        dev_of = ids_in // LOCAL_EXPERTS
        same_dev = dev_of[:, :, None] == dev_of[:, None, :]
        weights = jnp.where(same_dev, gate_in[:, None, :], 0.0)
        dev_sum = jnp.einsum('tjk,tkd->tjd', weights, outs_in.astype(jnp.float32)).astype(jnp.bfloat16)
        leader = jnp.logical_not(jnp.any(same_dev & earlier[None, :, :], axis=2))
        moe_sum = jnp.sum(jnp.where(leader[:, :, None], dev_sum.astype(jnp.float32), 0.0), axis=1)
        return (rows_in.astype(jnp.float32) + moe_sum).astype(jnp.bfloat16)

    output = lax.map(combine_block, (tokens.reshape(GROUP, TOK_DEV, D_MODEL), expert_ids.reshape(GROUP, TOK_DEV, TOP_K), gate_vals.reshape(GROUP, TOK_DEV, TOP_K), pair_out.reshape(GROUP, TOK_DEV, TOP_K, D_MODEL)))
    return output.reshape(TOKENS, D_MODEL)
```

```python
import functools

import jax
import jax.numpy as jnp
from jax import lax
from jax.experimental import pallas as pl
from jax.experimental.pallas import tpu as pltpu
from jax.sharding import PartitionSpec as P

MESH = pl.DeviceIdType.MESH
CORES = 2


def moe_kernel(groups, cap, x_ref, ids_ref, gates_ref, wg_hbm, wu_hbm, wd_hbm, out_ref,
               wg, wu, wd, chosen, pack, send, sgate, recv, rgate, gcol, hid, acc, ysend, yrecv, total,
               wsem, send_sem, recv_sem, gsend_sem, grecv_sem, ysend_sem, yrecv_sem):
    tok_dev, d_model = x_ref.shape
    local, _, ffn = wg.shape
    top_k = ids_ref.shape[0]
    lanes = sgate.shape[2]
    chips = groups // CORES
    f32, bf16 = jnp.float32, jnp.bfloat16
    me = lax.axis_index('ep')
    chip, core = me // CORES, me % CORES
    slots = [(0, 0), (0, 1)]
    near = [(d, 0) for d in (1, chips - 1)]
    far = [(d, c) for d in range(2, chips - 1) for c in range(CORES)]
    slots += near + far + [(d, 1) for d, _ in near]

    def peer(k, sign):
        dx, dc = slots[k]
        return lax.rem(chip + chips + sign * dx, chips) * CORES + lax.rem(core + dc, CORES)

    def weight_copies(e):
        return [pltpu.make_async_copy(src.at[e], dst.at[e], wsem.at[i, e])
                for i, (src, dst) in enumerate(((wg_hbm, wg), (wu_hbm, wu), (wd_hbm, wd)))]

    for e in range(local):
        for copy in weight_copies(e):
            copy.start()

    barrier = pltpu.get_barrier_semaphore()
    for k in range(1, groups):
        pl.semaphore_signal(barrier, inc=1, device_id={'ep': peer(k, 1)}, device_id_type=MESH)

    def rows(k):
        return pl.ds(k * cap, cap)

    def row_copy(k):
        return pltpu.make_async_remote_copy(
            src_ref=send.at[rows(k), :], dst_ref=recv.at[rows(k), :], send_sem=send_sem.at[k], recv_sem=recv_sem.at[k],
            device_id={'ep': peer(k, 1)}, device_id_type=MESH)

    def gate_copy(k):
        return pltpu.make_async_remote_copy(
            src_ref=sgate.at[k], dst_ref=rgate.at[k], send_sem=gsend_sem.at[k], recv_sem=grecv_sem.at[k],
            device_id={'ep': peer(k, 1)}, device_id_type=MESH)

    def back_copy(k):
        return pltpu.make_async_remote_copy(
            src_ref=ysend.at[rows(k), :], dst_ref=yrecv.at[rows(k), :], send_sem=ysend_sem.at[k], recv_sem=yrecv_sem.at[k],
            device_id={'ep': peer(k, -1)}, device_id_type=MESH)

    ids = ids_ref[...]
    gates = gates_ref[...]
    dev = ids // local
    for k in range(groups):
        chosen[k:k + 1, :] = jnp.max(jnp.where(dev == peer(k, 1), 1.0, 0.0), axis=0, keepdims=True)
    flags = chosen[...]
    earlier = lax.broadcasted_iota(jnp.int32, (tok_dev, tok_dev), 0) < lax.broadcasted_iota(jnp.int32, (tok_dev, tok_dev), 1)
    rank = jnp.dot(flags.astype(bf16), jnp.where(earlier, 1.0, 0.0).astype(bf16), preferred_element_type=f32)
    rank = jnp.where(flags > 0.0, rank, -1.0).astype(jnp.int32)
    row_id = lax.broadcasted_iota(jnp.int32, (lanes, tok_dev), 0)
    loc_id = lax.broadcasted_iota(jnp.int32, (local, tok_dev), 0)
    order = list(range(2, groups)) + [1, 0]
    for n, k in enumerate(order):
        onehot = jnp.where(row_id == rank[k:k + 1, :], 1.0, 0.0).astype(bf16)
        pack[rows(k), :] = onehot[:cap, :]
        packed = jnp.dot(onehot[:cap, :], x_ref[...], preferred_element_type=f32).astype(bf16)
        first = peer(k, 1) * local
        gate = jnp.zeros((local, tok_dev), f32)
        for j in range(top_k):
            gate += jnp.where(ids[j:j + 1, :] - first == loc_id, gates[j:j + 1, :], 0.0)
        high = gate.astype(bf16).astype(f32)
        mid = (gate - high).astype(bf16).astype(f32)
        low = gate - high - mid
        parts = jnp.concatenate([high, mid, low], axis=0).astype(bf16)
        moved = lax.dot_general(parts, onehot, (((1,), (1,)), ((), ())), preferred_element_type=f32)
        moved = moved[:local] + moved[local:2 * local] + moved[2 * local:]
        if k == 0:
            recv[rows(k), :] = packed
            rgate[k] = moved
        else:
            send[rows(k), :] = packed
            sgate[k] = moved
            if n == 0:
                pl.semaphore_wait(barrier, groups - 1)
            gate_copy(k).start()
            row_copy(k).start()

    pair = 2 * cap
    half = ffn // 2
    third = d_model // 3
    lane_id = lax.broadcasted_iota(jnp.int32, (pair, lanes), 1)

    def batch(b, carry):
        for i in range(groups // 2):
            @pl.when(b == i)
            def _(i=i):
                for k in (2 * i, 2 * i + 1):
                    if k > 0:
                        gate_copy(k).wait_recv()
                        row_copy(k).wait_recv()
                    gcol[(k % 2) * cap:(k % 2 + 1) * cap, :] = jnp.concatenate(
                        [rgate[k], jnp.zeros((lanes - local, lanes), f32)], axis=0).T[:cap, :]
        base = pl.multiple_of(b * pair, pair)

        def hidden(e):
            @pl.when(b == 0)
            def _():
                for copy in weight_copies(e)[:2]:
                    copy.wait()
            for n in range(2):
                cols = slice(n * half, (n + 1) * half)
                g = jnp.dot(recv[pl.ds(base, pair), :], wg[e, :, cols], preferred_element_type=f32)
                u = jnp.dot(recv[pl.ds(base, pair), :], wu[e, :, cols], preferred_element_type=f32)
                hid[lax.rem(e, 2), :, cols] = (jax.nn.silu(g) * u).astype(bf16)

        def wait_down(e):
            @pl.when(b == 0)
            def _():
                weight_copies(e)[2].wait()

        def down(e):
            gate = jnp.sum(jnp.where(lane_id == e, gcol[...], 0.0), axis=1, keepdims=True)
            for n in range(3):
                cols = slice(n * third, (n + 1) * third)
                y = jnp.dot(hid[lax.rem(e, 2)], wd[e, :, cols], preferred_element_type=f32).astype(bf16).astype(f32)
                acc[:, cols] += jnp.where(gate > 0.0, gate * y, 0.0)

        acc[...] = jnp.zeros_like(acc)
        hidden(0)

        def step(e, carry):
            wait_down(e - 1)
            hidden(e)
            down(e - 1)
            return carry

        lax.fori_loop(1, local, step, 0)
        wait_down(local - 1)
        down(local - 1)
        for i in range(groups // 2):
            @pl.when(b == i)
            def _(i=i):
                for k in (2 * i, 2 * i + 1):
                    part = acc[(k % 2) * cap:(k % 2 + 1) * cap, :].astype(bf16)
                    if k == 0:
                        yrecv[rows(k), :] = part
                    else:
                        ysend[rows(k), :] = part
                        back_copy(k).start()
        return carry

    lax.fori_loop(0, groups // 2, batch, 0)

    for i in range(groups // 2):
        for k in (2 * i, 2 * i + 1):
            if k > 0:
                back_copy(k).wait_recv()
        span = slice(i * pair, (i + 1) * pair)
        part = lax.dot_general(pack[span, :], yrecv[span, :], (((0,), (0,)), ((), ())), preferred_element_type=f32)
        if i == 0:
            total[...] = x_ref[...].astype(f32) + part
        elif i < groups // 2 - 1:
            total[...] += part
        else:
            out_ref[...] = (total[...] + part).astype(bf16)
    for k in range(1, groups):
        gate_copy(k).wait_send()
        row_copy(k).wait_send()
        back_copy(k).wait_send()


def solution(mesh):
    groups = mesh.shape['ep']
    row_spec = P(('dp', 'ep'))
    expert_spec = P('ep')

    def device_step(tokens, expert_ids, gate_vals, w_gate, w_up, w_down):
        tok_dev, top_k = expert_ids.shape
        d_model = tokens.shape[1]
        local, _, ffn = w_gate.shape
        cap = tok_dev * (top_k // 2) // groups
        lanes = 128
        f32, bf16 = jnp.float32, jnp.bfloat16
        vmem = pl.BlockSpec(memory_space=pltpu.VMEM)
        hbm = pl.BlockSpec(memory_space=pl.ANY)
        dma = pltpu.SemaphoreType.DMA((groups,))
        return pl.pallas_call(
            functools.partial(moe_kernel, groups, cap),
            out_shape=jax.ShapeDtypeStruct((tok_dev, d_model), bf16),
            in_specs=[vmem, vmem, vmem, hbm, hbm, hbm],
            out_specs=vmem,
            scratch_shapes=[
                pltpu.VMEM(w_gate.shape, bf16),
                pltpu.VMEM(w_up.shape, bf16),
                pltpu.VMEM(w_down.shape, bf16),
                pltpu.VMEM((groups, tok_dev), f32),
                pltpu.VMEM((groups * cap, tok_dev), bf16),
                pltpu.VMEM((groups * cap, d_model), bf16),
                pltpu.VMEM((groups, local, lanes), f32),
                pltpu.VMEM((groups * cap, d_model), bf16),
                pltpu.VMEM((groups, local, lanes), f32),
                pltpu.VMEM((2 * cap, lanes), f32),
                pltpu.VMEM((2, 2 * cap, ffn), bf16),
                pltpu.VMEM((2 * cap, d_model), f32),
                pltpu.VMEM((groups * cap, d_model), bf16),
                pltpu.VMEM((groups * cap, d_model), bf16),
                pltpu.VMEM((tok_dev, d_model), f32),
                pltpu.SemaphoreType.DMA((3, local)),
                dma, dma, dma, dma, dma, dma,
            ],
            compiler_params=pltpu.CompilerParams(collective_id=0, has_side_effects=True, vmem_limit_bytes=67043328),
        )(tokens, expert_ids.T, gate_vals.T, w_gate, w_up, w_down)

    return jax.shard_map(device_step, mesh=mesh, in_specs=(row_spec, row_spec, row_spec, expert_spec, expert_spec, expert_spec), out_specs=row_spec, check_vma=False)
```

```python
import contextlib
import functools

import jax
import jax.numpy as jnp
from jax import lax
from jax.experimental import pallas as pl
from jax.experimental.pallas import tpu as pltpu
from jax.sharding import PartitionSpec as P

MESH = pl.DeviceIdType.MESH
CORES = 2


def scope(name):
    return contextlib.nullcontext()


def moe_kernel(groups, cap, x_hbm, ids_hbm, gates_hbm, wg_hbm, wu_hbm, wd_hbm, out_ref,
               x_ref, ids_ref, gates_ref, wg, wu, wd, chosen, pack, send, sgate, recv, rgate, gcol, hid, acc, ysend, yrecv, total,
               isem, wsem, send_sem, recv_sem, gsend_sem, grecv_sem, ysend_sem, yrecv_sem):
    tok_dev, d_model = x_ref.shape
    local, _, ffn = wg.shape
    top_k = ids_ref.shape[0]
    lanes = sgate.shape[2]
    chips = groups // CORES
    f32, bf16 = jnp.float32, jnp.bfloat16
    me = lax.axis_index('ep')
    chip, core = me // CORES, me % CORES
    slots = [(d, c) for c in range(CORES) for d in (1, chips - 1)]
    slots += [(d, c) for d in range(2, chips - 1) for c in range(CORES)]
    slots += [(0, c) for c in range(CORES)]
    own = groups - CORES
    others = [k for k in range(groups) if k != own]

    def peer(k, sign):
        dx, dc = slots[k]
        return lax.rem(chip + chips + sign * dx, chips) * CORES + lax.rem(core + dc, CORES)

    def weight_copies(e):
        return [pltpu.make_async_copy(src.at[e], dst.at[e], wsem.at[i, e])
                for i, (src, dst) in enumerate(((wg_hbm, wg), (wu_hbm, wu), (wd_hbm, wd)))]

    barrier = pltpu.get_barrier_semaphore()
    for k in others:
        pl.semaphore_signal(barrier, inc=1, device_id={'ep': peer(k, 1)}, device_id_type=MESH)

    inputs = [pltpu.make_async_copy(src, dst, isem.at[i])
              for i, (src, dst) in enumerate(((ids_hbm, ids_ref), (gates_hbm, gates_ref), (x_hbm, x_ref)))]
    for copy in inputs:
        copy.start()

    def rows(k):
        return pl.ds(k * cap, cap)

    def row_copy(k):
        return pltpu.make_async_remote_copy(
            src_ref=send.at[rows(k), :], dst_ref=recv.at[rows(k), :], send_sem=send_sem.at[k], recv_sem=recv_sem.at[k],
            device_id={'ep': peer(k, 1)}, device_id_type=MESH)

    def gate_copy(k):
        return pltpu.make_async_remote_copy(
            src_ref=sgate.at[k], dst_ref=rgate.at[k], send_sem=gsend_sem.at[k], recv_sem=grecv_sem.at[k],
            device_id={'ep': peer(k, 1)}, device_id_type=MESH)

    def back_copy(k):
        return pltpu.make_async_remote_copy(
            src_ref=ysend.at[rows(k), :], dst_ref=yrecv.at[rows(k), :], send_sem=ysend_sem.at[k], recv_sem=yrecv_sem.at[k],
            device_id={'ep': peer(k, -1)}, device_id_type=MESH)

    inputs[0].wait()
    inputs[1].wait()
    ids = ids_ref[...]
    gates = gates_ref[...]
    dev = ids // local
    for k in range(groups):
        chosen[k:k + 1, :] = jnp.max(jnp.where(dev == peer(k, 1), 1.0, 0.0), axis=0, keepdims=True)
    flags = chosen[...]
    earlier = lax.broadcasted_iota(jnp.int32, (tok_dev, tok_dev), 0) < lax.broadcasted_iota(jnp.int32, (tok_dev, tok_dev), 1)
    rank = jnp.dot(flags.astype(bf16), jnp.where(earlier, 1.0, 0.0).astype(bf16), preferred_element_type=f32)
    rank = jnp.where(flags > 0.0, rank, -1.0).astype(jnp.int32)
    row_id = lax.broadcasted_iota(jnp.int32, (lanes, tok_dev), 0)
    loc_id = lax.broadcasted_iota(jnp.int32, (local, tok_dev), 0)
    inputs[2].wait()
    for e in range(local):
        for copy in weight_copies(e):
            copy.start()

    for n, k in enumerate(others + [own]):
        onehot = jnp.where(row_id == rank[k:k + 1, :], 1.0, 0.0).astype(bf16)
        pack[rows(k), :] = onehot[:cap, :]
        packed = jnp.dot(onehot[:cap, :], x_ref[...], preferred_element_type=f32).astype(bf16)
        first = peer(k, 1) * local
        gate = jnp.zeros((local, tok_dev), f32)
        for j in range(top_k):
            gate += jnp.where(ids[j:j + 1, :] - first == loc_id, gates[j:j + 1, :], 0.0)
        high = gate.astype(bf16).astype(f32)
        mid = (gate - high).astype(bf16).astype(f32)
        low = gate - high - mid
        parts = jnp.concatenate([high, mid, low], axis=0).astype(bf16)
        moved = lax.dot_general(parts, onehot, (((1,), (1,)), ((), ())), preferred_element_type=f32)
        moved = moved[:local] + moved[local:2 * local] + moved[2 * local:]
        if k == own:
            recv[rows(k), :] = packed
            rgate[k] = moved
        else:
            send[rows(k), :] = packed
            sgate[k] = moved
            if n == 0:
                with scope('barrier'):
                    pl.semaphore_wait(barrier, groups - 1)
            gate_copy(k).start()
            row_copy(k).start()

    pair = 2 * cap
    half = ffn // 2
    third = d_model // 3
    lane_id = lax.broadcasted_iota(jnp.int32, (pair, lanes), 1)

    def batch(b, carry):
        for i in range(groups // 2):
            @pl.when(b == i)
            def _(i=i):
                for k in (2 * i, 2 * i + 1):
                    if k != own:
                        with scope('rwait%d' % k):
                            gate_copy(k).wait_recv()
                            row_copy(k).wait_recv()
                    gcol[(k % 2) * cap:(k % 2 + 1) * cap, :] = jnp.concatenate(
                        [rgate[k], jnp.zeros((lanes - local, lanes), f32)], axis=0).T[:cap, :]
        base = pl.multiple_of(b * pair, pair)

        def hidden(e):
            for n in range(2):
                cols = slice(n * half, (n + 1) * half)
                g = jnp.dot(recv[pl.ds(base, pair), :], wg[e, :, cols], preferred_element_type=f32)
                u = jnp.dot(recv[pl.ds(base, pair), :], wu[e, :, cols], preferred_element_type=f32)
                hid[lax.rem(e, 2), :, cols] = (jax.nn.silu(g) * u).astype(bf16)

        def down(e):
            gate = jnp.sum(jnp.where(lane_id == e, gcol[...], 0.0), axis=1, keepdims=True)
            for n in range(3):
                cols = slice(n * third, (n + 1) * third)
                y = jnp.dot(hid[lax.rem(e, 2)], wd[e, :, cols], preferred_element_type=f32).astype(bf16).astype(f32)
                acc[:, cols] += jnp.where(gate > 0.0, gate * y, 0.0)

        with scope('first'):
            acc[...] = jnp.zeros_like(acc)
            hidden(0)

        def step(e, carry):
            hidden(e)
            down(e - 1)
            return carry

        with scope('steps'):
            lax.fori_loop(1, local, step, 0, unroll=True)
        with scope('last'):
            down(local - 1)
        for i in range(groups // 2):
            @pl.when(b == i)
            def _(i=i):
                for k in (2 * i, 2 * i + 1):
                    part = acc[(k % 2) * cap:(k % 2 + 1) * cap, :].astype(bf16)
                    if k == own:
                        yrecv[rows(k), :] = part
                    else:
                        ysend[rows(k), :] = part
                        back_copy(k).start()
        return carry

    for e in range(local):
        for copy in weight_copies(e):
            copy.wait()
    lax.fori_loop(0, groups // 2, batch, 0)

    tail = list(range(groups // 2))
    tail[-2:] = tail[:-3:-1]
    for n, i in enumerate(tail):
        for k in (2 * i, 2 * i + 1):
            if k != own:
                with scope('ywait%d' % k):
                    back_copy(k).wait_recv()
        span = slice(i * pair, (i + 1) * pair)
        part = lax.dot_general(pack[span, :], yrecv[span, :], (((0,), (0,)), ((), ())), preferred_element_type=f32)
        if n == 0:
            total[...] = x_ref[...].astype(f32) + part
        elif n < len(tail) - 1:
            total[...] += part
        else:
            out_ref[...] = (total[...] + part).astype(bf16)
    with scope('sends'):
        for k in others:
            gate_copy(k).wait_send()
            row_copy(k).wait_send()
            back_copy(k).wait_send()


def solution(mesh):
    groups = mesh.shape['ep']
    row_spec = P(('dp', 'ep'))
    expert_spec = P('ep')

    def device_step(tokens, expert_ids, gate_vals, w_gate, w_up, w_down):
        tok_dev, top_k = expert_ids.shape
        d_model = tokens.shape[1]
        local, _, ffn = w_gate.shape
        cap = tok_dev * (top_k // 2) // groups
        lanes = 128
        f32, bf16 = jnp.float32, jnp.bfloat16
        vmem = pl.BlockSpec(memory_space=pltpu.VMEM)
        hbm = pl.BlockSpec(memory_space=pl.ANY)
        dma = pltpu.SemaphoreType.DMA((groups,))
        return pl.pallas_call(
            functools.partial(moe_kernel, groups, cap),
            out_shape=pltpu.VMEM((tok_dev, d_model), bf16),
            in_specs=[hbm] * 6,
            out_specs=vmem,
            scratch_shapes=[
                pltpu.VMEM(tokens.shape, bf16),
                pltpu.VMEM((top_k, tok_dev), jnp.int32),
                pltpu.VMEM((top_k, tok_dev), f32),
                pltpu.VMEM(w_gate.shape, bf16),
                pltpu.VMEM(w_up.shape, bf16),
                pltpu.VMEM(w_down.shape, bf16),
                pltpu.VMEM((groups, tok_dev), f32),
                pltpu.VMEM((groups * cap, tok_dev), bf16),
                pltpu.VMEM((groups * cap, d_model), bf16),
                pltpu.VMEM((groups, local, lanes), f32),
                pltpu.VMEM((groups * cap, d_model), bf16),
                pltpu.VMEM((groups, local, lanes), f32),
                pltpu.VMEM((2 * cap, lanes), f32),
                pltpu.VMEM((2, 2 * cap, ffn), bf16),
                pltpu.VMEM((2 * cap, d_model), f32),
                pltpu.VMEM((groups * cap, d_model), bf16),
                pltpu.VMEM((groups * cap, d_model), bf16),
                pltpu.VMEM((tok_dev, d_model), f32),
                pltpu.SemaphoreType.DMA((3,)),
                pltpu.SemaphoreType.DMA((3, local)),
                dma, dma, dma, dma, dma, dma,
            ],
            compiler_params=pltpu.CompilerParams(collective_id=0, has_side_effects=True, vmem_limit_bytes=54 * 1024 * 1024),
        )(tokens, expert_ids.T, gate_vals.T, w_gate, w_up, w_down)

    return jax.shard_map(device_step, mesh=mesh, in_specs=(row_spec, row_spec, row_spec, expert_spec, expert_spec, expert_spec), out_specs=row_spec, check_vma=False)
```

```python
import contextlib
import functools

import jax
import jax.numpy as jnp
from jax import lax
from jax.experimental import pallas as pl
from jax.experimental.pallas import tpu as pltpu
from jax.sharding import PartitionSpec as P

MESH = pl.DeviceIdType.MESH
CORES = 2


def scope(name):
    return contextlib.nullcontext()


def moe_kernel(groups, cap, x_hbm, ids_hbm, gates_hbm, wg_hbm, wu_hbm, wd_hbm, out_ref,
               x_ref, ids_ref, gates_ref, wg, wu, wd, chosen, rank, rrank, raw, pack, send, sgate, recv, rgate, gcol, hid, acc, ysend, yrecv, total,
               isem, wsem, raw_sem, send_sem, recv_sem, gsend_sem, grecv_sem, ysend_sem, yrecv_sem):
    tok_dev, d_model = x_ref.shape
    local, _, ffn = wg.shape
    top_k = ids_ref.shape[0]
    lanes = sgate.shape[2]
    chips = groups // CORES
    f32, bf16 = jnp.float32, jnp.bfloat16
    me = lax.axis_index('ep')
    chip, core = me // CORES, me % CORES
    side = 1 - 2 * core
    dests = [(side, 0), (side, 1), (-side, 0), (chips // 2, 0), (-side, 1), (chips // 2, 1), (0, 0), (0, 1)]
    homes = [(-side, 0), (side, 1), (side, 0), (chips // 2, 0), (-side, 1), (chips // 2, 1), (0, 0), (0, 1)]
    direct, relayed, own = (2, 4), (1, 3, 5), 6
    others = [k for k in range(groups) if k != own]

    def device(dx, dc):
        return lax.rem(chip + chips + dx, chips) * CORES + lax.rem(core + dc, CORES)

    def weight_copies(e):
        return [pltpu.make_async_copy(src.at[e], dst.at[e], wsem.at[i, e])
                for i, (src, dst) in enumerate(((wg_hbm, wg), (wu_hbm, wu), (wd_hbm, wd)))]

    barrier = pltpu.get_barrier_semaphore()
    for k in others:
        pl.semaphore_signal(barrier, inc=1, device_id={'ep': device(*dests[k])}, device_id_type=MESH)

    inputs = [pltpu.make_async_copy(src, dst, isem.at[i])
              for i, (src, dst) in enumerate(((ids_hbm, ids_ref), (gates_hbm, gates_ref), (x_hbm, x_ref)))]
    for copy in inputs:
        copy.start()

    def rows(k):
        return pl.ds(k * cap, cap)

    def remote(src, dst, sems, to):
        return pltpu.make_async_remote_copy(
            src_ref=src, dst_ref=dst, send_sem=sems[0], recv_sem=sems[1], device_id={'ep': device(*to)}, device_id_type=MESH)

    def row_copy(k):
        to = {1: (0, 1), 3: (side, 0), 5: (side, 1)}.get(k, dests[k])
        return remote(send.at[rows(k), :], recv.at[rows(k), :], (send_sem.at[k], recv_sem.at[k]), to)

    def gate_copy(k):
        return remote(sgate.at[k], rgate.at[k], (gsend_sem.at[k], grecv_sem.at[k]), dests[k])

    def back_copy(k):
        return remote(ysend.at[rows(k), :], yrecv.at[rows(k), :], (ysend_sem.at[k], yrecv_sem.at[k]), homes[k])

    raw_copy = remote(x_ref, raw, (raw_sem.at[0], raw_sem.at[1]), (side, 0))
    rank_copy = remote(rank, rrank, (raw_sem.at[2], raw_sem.at[3]), (side, 0))

    inputs[2].wait()
    with scope('barrier'):
        pl.semaphore_wait(barrier, groups - 1)
    raw_copy.start()

    inputs[0].wait()
    inputs[1].wait()
    ids = ids_ref[...]
    gates = gates_ref[...]
    dev = ids // local
    for k in range(groups):
        chosen[k:k + 1, :] = jnp.max(jnp.where(dev == device(*dests[k]), 1.0, 0.0), axis=0, keepdims=True)
    flags = chosen[...]
    earlier = lax.broadcasted_iota(jnp.int32, (tok_dev, tok_dev), 0) < lax.broadcasted_iota(jnp.int32, (tok_dev, tok_dev), 1)
    order = jnp.dot(flags.astype(bf16), jnp.where(earlier, 1.0, 0.0).astype(bf16), preferred_element_type=f32)
    rank[...] = jnp.where(flags > 0.0, order, -1.0).astype(jnp.int32)
    rank_copy.start()
    for e in range(local):
        for copy in weight_copies(e):
            copy.start()

    row_id = lax.broadcasted_iota(jnp.int32, (lanes, tok_dev), 0)
    loc_id = lax.broadcasted_iota(jnp.int32, (local, tok_dev), 0)
    for k in (7, 2, 4, 6, 0, 1, 3, 5):
        onehot = jnp.where(row_id == rank[k:k + 1, :], 1.0, 0.0).astype(bf16)
        pack[rows(k), :] = onehot[:cap, :]
        first = device(*dests[k]) * local
        gate = jnp.zeros((local, tok_dev), f32)
        for j in range(top_k):
            gate += jnp.where(ids[j:j + 1, :] - first == loc_id, gates[j:j + 1, :], 0.0)
        high = gate.astype(bf16).astype(f32)
        mid = (gate - high).astype(bf16).astype(f32)
        low = gate - high - mid
        parts = jnp.concatenate([high, mid, low], axis=0).astype(bf16)
        moved = lax.dot_general(parts, onehot, (((1,), (1,)), ((), ())), preferred_element_type=f32)
        moved = moved[:local] + moved[local:2 * local] + moved[2 * local:]
        if k == own:
            rgate[k] = moved
        else:
            sgate[k] = moved
            gate_copy(k).start()
        if k in direct + (7, own):
            packed = jnp.dot(onehot[:cap, :], x_ref[...], preferred_element_type=f32).astype(bf16)
            if k == own:
                recv[rows(k), :] = packed
            else:
                send[rows(k), :] = packed
                if k == 7:
                    row_copy(k).start()
    with scope('rawsend'):
        raw_copy.wait_send()
    for k in direct:
        row_copy(k).start()
    with scope('rawwait'):
        rank_copy.wait_recv()
        raw_copy.wait_recv()
    with scope('relay'):
        for k in (1, 3, 5, 0):
            onehot = jnp.where(row_id[:cap, :] == rrank[k:k + 1, :], 1.0, 0.0).astype(bf16)
            packed = jnp.dot(onehot, raw[...], preferred_element_type=f32).astype(bf16)
            if k == 0:
                recv[rows(k), :] = packed
            else:
                send[rows(k), :] = packed
                row_copy(k).start()

    pair = 2 * cap
    half = ffn // 2
    third = d_model // 3
    lane_id = lax.broadcasted_iota(jnp.int32, (pair, lanes), 1)

    def batch(b, carry):
        for i in range(groups // 2):
            @pl.when(b == i)
            def _(i=i):
                for k in (2 * i, 2 * i + 1):
                    if k != own:
                        with scope('rwait%d' % k):
                            gate_copy(k).wait_recv()
                            if k > 0:
                                row_copy(k).wait_recv()
                    gcol[(k % 2) * cap:(k % 2 + 1) * cap, :] = jnp.concatenate(
                        [rgate[k], jnp.zeros((lanes - local, lanes), f32)], axis=0).T[:cap, :]
        base = pl.multiple_of(b * pair, pair)

        def hidden(e):
            for n in range(2):
                cols = slice(n * half, (n + 1) * half)
                g = jnp.dot(recv[pl.ds(base, pair), :], wg[e, :, cols], preferred_element_type=f32)
                u = jnp.dot(recv[pl.ds(base, pair), :], wu[e, :, cols], preferred_element_type=f32)
                hid[lax.rem(e, 2), :, cols] = (jax.nn.silu(g) * u).astype(bf16)

        def down(e):
            gate = jnp.sum(jnp.where(lane_id == e, gcol[...], 0.0), axis=1, keepdims=True)
            for n in range(3):
                cols = slice(n * third, (n + 1) * third)
                y = jnp.dot(hid[lax.rem(e, 2)], wd[e, :, cols], preferred_element_type=f32).astype(bf16).astype(f32)
                acc[:, cols] += jnp.where(gate > 0.0, gate * y, 0.0)

        with scope('first'):
            acc[...] = jnp.zeros_like(acc)
            hidden(0)

        def step(e, carry):
            hidden(e)
            down(e - 1)
            return carry

        with scope('steps'):
            lax.fori_loop(1, local, step, 0, unroll=True)
        with scope('last'):
            down(local - 1)
        for i in range(groups // 2):
            @pl.when(b == i)
            def _(i=i):
                for k in (2 * i + 1, 2 * i):
                    part = acc[(k % 2) * cap:(k % 2 + 1) * cap, :].astype(bf16)
                    if k == own:
                        yrecv[rows(k), :] = part
                    else:
                        ysend[rows(k), :] = part
                        back_copy(k).start()
        return carry

    for e in range(local):
        for copy in weight_copies(e):
            copy.wait()
    lax.fori_loop(0, groups // 2, batch, 0)

    tail = list(range(groups // 2))
    tail[-2:] = tail[:-3:-1]
    for n, i in enumerate(tail):
        for k in (2 * i, 2 * i + 1):
            if k != own:
                with scope('ywait%d' % k):
                    back_copy(k).wait_recv()
        span = slice(i * pair, (i + 1) * pair)
        part = lax.dot_general(pack[span, :], yrecv[span, :], (((0,), (0,)), ((), ())), preferred_element_type=f32)
        if n == 0:
            total[...] = x_ref[...].astype(f32) + part
        elif n < len(tail) - 1:
            total[...] += part
        else:
            out_ref[...] = (total[...] + part).astype(bf16)
    with scope('sends'):
        for k in others:
            gate_copy(k).wait_send()
            if k > 0:
                row_copy(k).wait_send()
            back_copy(k).wait_send()
        rank_copy.wait_send()


def solution(mesh):
    groups = mesh.shape['ep']
    row_spec = P(('dp', 'ep'))
    expert_spec = P('ep')

    def device_step(tokens, expert_ids, gate_vals, w_gate, w_up, w_down):
        tok_dev, top_k = expert_ids.shape
        d_model = tokens.shape[1]
        local, _, ffn = w_gate.shape
        cap = tok_dev * (top_k // 2) // groups
        lanes = 128
        f32, bf16 = jnp.float32, jnp.bfloat16
        vmem = pl.BlockSpec(memory_space=pltpu.VMEM)
        hbm = pl.BlockSpec(memory_space=pl.ANY)
        dma = pltpu.SemaphoreType.DMA((groups,))
        return pl.pallas_call(
            functools.partial(moe_kernel, groups, cap),
            out_shape=pltpu.VMEM((tok_dev, d_model), bf16),
            in_specs=[hbm] * 6,
            out_specs=vmem,
            scratch_shapes=[
                pltpu.VMEM(tokens.shape, bf16),
                pltpu.VMEM((top_k, tok_dev), jnp.int32),
                pltpu.VMEM((top_k, tok_dev), f32),
                pltpu.VMEM(w_gate.shape, bf16),
                pltpu.VMEM(w_up.shape, bf16),
                pltpu.VMEM(w_down.shape, bf16),
                pltpu.VMEM((groups, tok_dev), f32),
                pltpu.VMEM((groups, tok_dev), jnp.int32),
                pltpu.VMEM((groups, tok_dev), jnp.int32),
                pltpu.VMEM(tokens.shape, bf16),
                pltpu.VMEM((groups * cap, tok_dev), bf16),
                pltpu.VMEM((groups * cap, d_model), bf16),
                pltpu.VMEM((groups, local, lanes), f32),
                pltpu.VMEM((groups * cap, d_model), bf16),
                pltpu.VMEM((groups, local, lanes), f32),
                pltpu.VMEM((2 * cap, lanes), f32),
                pltpu.VMEM((2, 2 * cap, ffn), bf16),
                pltpu.VMEM((2 * cap, d_model), f32),
                pltpu.VMEM((groups * cap, d_model), bf16),
                pltpu.VMEM((groups * cap, d_model), bf16),
                pltpu.VMEM((tok_dev, d_model), f32),
                pltpu.SemaphoreType.DMA((3,)),
                pltpu.SemaphoreType.DMA((3, local)),
                pltpu.SemaphoreType.DMA((4,)),
                dma, dma, dma, dma, dma, dma,
            ],
            compiler_params=pltpu.CompilerParams(collective_id=0, has_side_effects=True, vmem_limit_bytes=54 * 1024 * 1024),
        )(tokens, expert_ids.T, gate_vals.T, w_gate, w_up, w_down)

    return jax.shard_map(device_step, mesh=mesh, in_specs=(row_spec, row_spec, row_spec, expert_spec, expert_spec, expert_spec), out_specs=row_spec, check_vma=False)
```

```python
import contextlib
import functools

import jax
import jax.numpy as jnp
from jax import lax
from jax.experimental import pallas as pl
from jax.experimental.pallas import tpu as pltpu
from jax.sharding import PartitionSpec as P

MESH = pl.DeviceIdType.MESH
CORES = 2


def scope(name):
    return contextlib.nullcontext()


def moe_kernel(groups, cap, x_hbm, ids_hbm, gates_hbm, wg_hbm, wu_hbm, wd_hbm, out_ref,
               x_ref, ids_ref, gates_ref, wg, wu, wd, chosen, rank, rrank, raw, rpack, pack, send, sgate, recv, rgate,
               gcol, hid, acc, ysend, yrecv, total,
               in_sem, w_sem, raw_send, raw_recv, rank_sem, row_send, row_recv, gate_sem, back_send, back_recv):
    tok_dev, d_model = x_ref.shape
    local, _, ffn = wg.shape
    top_k = ids_ref.shape[0]
    lanes = sgate.shape[2]
    chips = groups // CORES
    batches = groups // 2
    pair = 2 * cap
    f32, bf16 = jnp.float32, jnp.bfloat16
    me = lax.axis_index('ep')
    chip, core = me // CORES, me % CORES
    side = 1 - 2 * core
    dests = [(side, 0), (side, 1), (-side, 0), (chips // 2, 0), (-side, 1), (chips // 2, 1), (0, 0), (0, 1)]
    homes = [(-side, 0), (side, 1), (side, 0), (chips // 2, 0), (-side, 1), (chips // 2, 1), (0, 0), (0, 1)]
    direct, near, own, partner = (2, 4), (1, 0, 3, 5), 6, 7
    relay_to = {1: (0, 1), 3: (side, 0), 5: (side, 1)}
    others = [k for k in range(groups) if k != own]

    def device(dx, dc):
        return lax.rem(chip + chips + dx, chips) * CORES + lax.rem(core + dc, CORES)

    def remote(src, dst, send_sem, recv_sem, to):
        return pltpu.make_async_remote_copy(
            src_ref=src, dst_ref=dst, send_sem=send_sem, recv_sem=recv_sem, device_id={'ep': device(*to)}, device_id_type=MESH)

    def rows(k, count=1):
        return pl.ds(k * cap, count * cap)

    barrier = pltpu.get_barrier_semaphore()
    for k in others:
        pl.semaphore_signal(barrier, inc=1, device_id={'ep': device(*dests[k])}, device_id_type=MESH)

    inputs = [pltpu.make_async_copy(src, dst, in_sem.at[i])
              for i, (src, dst) in enumerate(((ids_hbm, ids_ref), (gates_hbm, gates_ref), (x_hbm, x_ref)))]
    weights = [pltpu.make_async_copy(src, dst, w_sem.at[i])
               for i, (src, dst) in enumerate(((wg_hbm, wg), (wu_hbm, wu), (wd_hbm, wd)))]

    early = d_model // 2
    tail_cols = lanes
    halves = [slice(0, early), slice(early, d_model)]
    chunks = [(slice(0, early), 0, 0), (slice(early, d_model - tail_cols), 0, 1), (slice(d_model - tail_cols, d_model), 1, 1)]
    raw_copies = [remote(x_ref.at[:, cols], raw.at[:, cols], raw_send.at[i], raw_recv.at[j], (side, 0)) for cols, i, j in chunks]
    sent_cols = [slice(0, d_model - tail_cols), slice(d_model - tail_cols, d_model)]
    raw_sent = [remote(x_ref.at[:, cols], raw.at[:, cols], raw_send.at[i], raw_recv.at[0], (side, 0)) for i, cols in enumerate(sent_cols)]
    raw_came = [remote(x_ref.at[:, cols], raw.at[:, cols], raw_send.at[0], raw_recv.at[j], (side, 0)) for j, cols in enumerate(halves)]
    rank_copy = remote(rank, rrank, rank_sem.at[0], rank_sem.at[1], (side, 0))

    def row_copies(k):
        pieces = halves if k in relay_to else [slice(0, d_model)]
        return [remote(send.at[rows(k), cols], recv.at[rows(k), cols], row_send.at[0], row_recv.at[k // 2], relay_to.get(k, dests[k]))
                for cols in pieces]

    def gate_copy(k):
        return remote(sgate.at[k], rgate.at[k], gate_sem.at[0], gate_sem.at[1], dests[k])

    def back_copy(k):
        return remote(ysend.at[rows(k), :], yrecv.at[rows(k), :], back_send.at[0], back_recv.at[k // 2], homes[k])

    def wait_rows(i):
        first, count = {0: (1, 1), batches - 1: (partner, 1)}.get(i, (2 * i, 2))
        remote(send.at[rows(first, count), :], recv.at[rows(first, count), :], row_send.at[0], row_recv.at[i], (0, 1)).wait_recv()

    def wait_back(i):
        first, count = (partner, 1) if i == batches - 1 else (2 * i, 2)
        remote(ysend.at[rows(first, count), :], yrecv.at[rows(first, count), :], back_send.at[0], back_recv.at[i], (0, 1)).wait_recv()

    for copy in inputs:
        copy.start()
    inputs[2].wait()
    for copy in weights:
        copy.start()
    with scope('barrier'):
        pl.semaphore_wait(barrier, groups - 1)
    raw_copies[0].start()

    inputs[0].wait()
    inputs[1].wait()
    ids = ids_ref[...]
    gates = gates_ref[...]
    dev = ids // local
    for k in range(groups):
        chosen[k:k + 1, :] = jnp.max(jnp.where(dev == device(*dests[k]), 1.0, 0.0), axis=0, keepdims=True)
    flags = chosen[...]
    earlier = lax.broadcasted_iota(jnp.int32, (tok_dev, tok_dev), 0) < lax.broadcasted_iota(jnp.int32, (tok_dev, tok_dev), 1)
    order = jnp.dot(flags.astype(bf16), jnp.where(earlier, 1.0, 0.0).astype(bf16), preferred_element_type=f32)
    rank[...] = jnp.where(flags > 0.0, order, -1.0).astype(jnp.int32)
    rank_copy.start()

    row_id = lax.broadcasted_iota(jnp.int32, (lanes, tok_dev), 0)
    loc_id = lax.broadcasted_iota(jnp.int32, (local, tok_dev), 0)
    for k in (7, 2, 4, 6, 0, 1, 3, 5):
        onehot = jnp.where(row_id == rank[k:k + 1, :], 1.0, 0.0).astype(bf16)
        pack[rows(k), :] = onehot[:cap, :]
        first = device(*dests[k]) * local
        gate = jnp.zeros((local, tok_dev), f32)
        for j in range(top_k):
            gate += jnp.where(ids[j:j + 1, :] - first == loc_id, gates[j:j + 1, :], 0.0)
        high = gate.astype(bf16).astype(f32)
        mid = (gate - high).astype(bf16).astype(f32)
        low = gate - high - mid
        parts = jnp.concatenate([high, mid, low], axis=0).astype(bf16)
        moved = lax.dot_general(parts, onehot, (((1,), (1,)), ((), ())), preferred_element_type=f32)
        moved = moved[:local] + moved[local:2 * local] + moved[2 * local:]
        if k == own:
            rgate[groups] = moved
        else:
            sgate[k] = moved
    for k in others:
        gate_copy(k).start()
    for copy in raw_copies[1:]:
        copy.start()
    for k in (partner,) + direct + (own,):
        packed = jnp.dot(pack[rows(k), :], x_ref[...], preferred_element_type=f32).astype(bf16)
        if k == own:
            recv[rows(k), :] = packed
        else:
            send[rows(k), :] = packed
            if k == partner:
                for copy in row_copies(k):
                    copy.start()

    with scope('rankwait'):
        rank_copy.wait_recv()
    for i, k in enumerate(near):
        rpack[i * cap:(i + 1) * cap, :] = jnp.where(row_id[:cap, :] == rrank[k:k + 1, :], 1.0, 0.0).astype(bf16)

    def relay(i, h):
        k, cols = near[i], halves[h]
        packed = jnp.dot(rpack[i * cap:(i + 1) * cap, :], raw[:, cols], preferred_element_type=f32).astype(bf16)
        if k == 0:
            recv[rows(k), cols] = packed
        else:
            send[rows(k), cols] = packed

    with scope('raw0'):
        raw_came[0].wait_recv()
    with scope('relay0'):
        for i in range(4):
            relay(i, 0)
        row_copies(1)[0].start()
    with scope('gates'):
        remote(sgate.at[pl.ds(0, groups - 1)], rgate.at[pl.ds(0, groups - 1)], gate_sem.at[0], gate_sem.at[1], (0, 1)).wait_recv()
        for k in range(groups):
            mine = rgate[groups if k == own else k]
            gcol[k // 2, (k % 2) * cap:(k % 2 + 1) * cap, :] = jnp.concatenate(
                [mine, jnp.zeros((lanes - local, lanes), f32)], axis=0).T[:cap, :]
    with scope('rawsend'):
        raw_sent[0].wait_send()
        raw_sent[1].wait_send()
    for k in direct + (3,):
        row_copies(k)[0].start()
    with scope('raw1'):
        raw_came[1].wait_recv()
    with scope('relay1'):
        for i, k in enumerate(near):
            relay(i, 1)
            if k == 5:
                row_copies(k)[0].start()
            if k > 0:
                row_copies(k)[1].start()

    half = ffn // 2
    third = d_model // 3
    lane_id = lax.broadcasted_iota(jnp.int32, (pair, lanes), 1)

    def hidden(e, base):
        for n in range(2):
            cols = slice(n * half, (n + 1) * half)
            g = jnp.dot(recv[pl.ds(base, pair), :], wg[e, :, cols], preferred_element_type=f32)
            u = jnp.dot(recv[pl.ds(base, pair), :], wu[e, :, cols], preferred_element_type=f32)
            hid[e % 2, :, cols] = (jax.nn.silu(g) * u).astype(bf16)

    def down(e, b, base):
        gate = jnp.sum(jnp.where(lane_id == e, gcol[b], 0.0), axis=1, keepdims=True)
        for n in range(3):
            cols = slice(n * third, (n + 1) * third)
            y = jnp.dot(hid[e % 2], wd[e, :, cols], preferred_element_type=f32).astype(bf16).astype(f32)
            y = jnp.where(gate > 0.0, gate * y, 0.0)
            if e == 0:
                acc[:, cols] = y
            elif e < local - 1:
                acc[:, cols] += y
            else:
                ysend[pl.ds(base, pair), cols] = (acc[:, cols] + y).astype(bf16)

    def batch(b, carry):
        base = pl.multiple_of(b * pair, pair)
        for i in range(batches):
            @pl.when(b == i)
            def _(i=i):
                with scope('rwait%d' % i):
                    wait_rows(i)
        with scope('steps'):
            hidden(0, base)
            for e in range(1, local):
                hidden(e, base)
                down(e - 1, b, base)
            down(local - 1, b, base)
        for i in range(batches):
            @pl.when(b == i)
            def _(i=i):
                for k in (2 * i + 1, 2 * i):
                    if k == own:
                        yrecv[rows(k), :] = ysend[rows(k), :]
                    else:
                        back_copy(k).start()
        return carry

    with scope('weights'):
        for copy in weights:
            copy.wait()
    lax.fori_loop(0, batches, batch, 0)

    ends = list(range(batches))
    ends[-2:] = ends[:-3:-1]
    for n, i in enumerate(ends):
        with scope('ywait%d' % i):
            wait_back(i)
        span = slice(i * pair, (i + 1) * pair)
        part = lax.dot_general(pack[span, :], yrecv[span, :], (((0,), (0,)), ((), ())), preferred_element_type=f32)
        if n == 0:
            total[...] = x_ref[...].astype(f32) + part
        elif n < batches - 1:
            total[...] += part
        else:
            out_ref[...] = (total[...] + part).astype(bf16)
    with scope('sends'):
        rank_copy.wait_send()
        remote(send.at[pl.ds(0, 6 * cap), :], recv.at[pl.ds(0, 6 * cap), :], row_send.at[0], row_recv.at[0], (0, 1)).wait_send()
        remote(sgate.at[pl.ds(0, groups - 1)], rgate.at[pl.ds(0, groups - 1)], gate_sem.at[0], gate_sem.at[1], (0, 1)).wait_send()
        remote(ysend.at[rows(0, groups - 1), :], yrecv.at[rows(0, groups - 1), :], back_send.at[0], back_recv.at[0], (0, 1)).wait_send()


def solution(mesh):
    groups = mesh.shape['ep']
    row_spec = P(('dp', 'ep'))
    expert_spec = P('ep')

    def device_step(tokens, expert_ids, gate_vals, w_gate, w_up, w_down):
        tok_dev, top_k = expert_ids.shape
        d_model = tokens.shape[1]
        local, _, ffn = w_gate.shape
        cap = tok_dev * (top_k // 2) // groups
        lanes = 128
        f32, bf16 = jnp.float32, jnp.bfloat16
        slots = groups * cap
        dma = pltpu.SemaphoreType.DMA
        return pl.pallas_call(
            functools.partial(moe_kernel, groups, cap),
            out_shape=pltpu.VMEM((tok_dev, d_model), bf16),
            in_specs=[pl.BlockSpec(memory_space=pl.ANY)] * 6,
            out_specs=pl.BlockSpec(memory_space=pltpu.VMEM),
            scratch_shapes=[
                pltpu.VMEM(tokens.shape, bf16),
                pltpu.VMEM((top_k, tok_dev), jnp.int32),
                pltpu.VMEM((top_k, tok_dev), f32),
                pltpu.VMEM(w_gate.shape, bf16),
                pltpu.VMEM(w_up.shape, bf16),
                pltpu.VMEM(w_down.shape, bf16),
                pltpu.VMEM((groups, tok_dev), f32),
                pltpu.VMEM((groups, tok_dev), jnp.int32),
                pltpu.VMEM((groups, tok_dev), jnp.int32),
                pltpu.VMEM(tokens.shape, bf16),
                pltpu.VMEM((slots // 2, tok_dev), bf16),
                pltpu.VMEM((slots, tok_dev), bf16),
                pltpu.VMEM((slots, d_model), bf16),
                pltpu.VMEM((groups, local, lanes), f32),
                pltpu.VMEM((slots, d_model), bf16),
                pltpu.VMEM((groups + 1, local, lanes), f32),
                pltpu.VMEM((groups // 2, 2 * cap, lanes), f32),
                pltpu.VMEM((2, 2 * cap, ffn), bf16),
                pltpu.VMEM((2 * cap, d_model), f32),
                pltpu.VMEM((slots, d_model), bf16),
                pltpu.VMEM((slots, d_model), bf16),
                pltpu.VMEM((tok_dev, d_model), f32),
                dma((3,)), dma((3,)), dma((2,)), dma((2,)), dma((2,)),
                dma((1,)), dma((groups // 2,)), dma((2,)), dma((1,)), dma((groups // 2,)),
            ],
            compiler_params=pltpu.CompilerParams(collective_id=0, has_side_effects=True, vmem_limit_bytes=56 * 1024 * 1024),
        )(tokens, expert_ids.T, gate_vals.T, w_gate, w_up, w_down)

    return jax.shard_map(device_step, mesh=mesh, in_specs=(row_spec, row_spec, row_spec, expert_spec, expert_spec, expert_spec), out_specs=row_spec, check_vma=False)
```

```python
import contextlib
import functools

import jax
import jax.numpy as jnp
from jax import lax
from jax.experimental import pallas as pl
from jax.experimental.pallas import tpu as pltpu
from jax.sharding import PartitionSpec as P

MESH = pl.DeviceIdType.MESH
CORES = 2


def scope(name):
    return contextlib.nullcontext()


def moe_kernel(groups, cap, x_hbm, ids_hbm, gates_hbm, wg_hbm, wu_hbm, wd_hbm, out_ref,
               x_ref, ids_ref, gates_ref, wg, wu, wd, chosen, rank, nrank, rrank, raw, rpack, pack, send, sgate, recv, rgate,
               gcol, hid, acc, ysend, yrecv, total,
               in_sem, w_sem, raw_send, raw_recv, rank_sem, row_send, row_recv, gate_sem, back_send, back_recv, known):
    tok_dev, d_model = x_ref.shape
    local, _, ffn = wg.shape
    top_k = ids_ref.shape[0]
    lanes = sgate.shape[2]
    chips = groups // CORES
    batches = groups // 2
    pair = 2 * cap
    f32, bf16 = jnp.float32, jnp.bfloat16
    me = lax.axis_index('ep')
    chip, core = me // CORES, me % CORES
    side = 1 - 2 * core
    dests = [(side, 0), (side, 1), (-side, 0), (chips // 2, 0), (-side, 1), (chips // 2, 1), (0, 0), (0, 1)]
    homes = [(-side, 0), (side, 1), (side, 0), (chips // 2, 0), (-side, 1), (chips // 2, 1), (0, 0), (0, 1)]
    direct, near, own, partner = (2, 4), (1, 0, 3, 5), 6, 7
    relay_to = {1: (0, 1), 3: (side, 0), 5: (side, 1)}
    others = [k for k in range(groups) if k != own]

    def device(dx, dc):
        return lax.rem(chip + chips + dx, chips) * CORES + lax.rem(core + dc, CORES)

    def remote(src, dst, send_sem, recv_sem, to):
        return pltpu.make_async_remote_copy(
            src_ref=src, dst_ref=dst, send_sem=send_sem, recv_sem=recv_sem, device_id={'ep': device(*to)}, device_id_type=MESH)

    def rows(k, count=1):
        return pl.ds(k * cap, count * cap)

    def tell(sem, to):
        pl.semaphore_signal(sem, inc=1, device_id={'ep': device(*to)}, device_id_type=MESH)

    barrier = pltpu.get_barrier_semaphore()
    tell(barrier, (-side, 0))
    tell(barrier, (0, 1))

    inputs = [pltpu.make_async_copy(src, dst, in_sem.at[i])
              for i, (src, dst) in enumerate(((ids_hbm, ids_ref), (gates_hbm, gates_ref), (x_hbm, x_ref)))]
    weights = [pltpu.make_async_copy(src, dst, w_sem.at[i])
               for i, (src, dst) in enumerate(((wg_hbm, wg), (wu_hbm, wu), (wd_hbm, wd)))]

    early = d_model // 2
    halves = [slice(0, early), slice(early, d_model)]
    raw_copies = [remote(x_ref.at[:, cols], raw.at[:, cols], raw_send.at[h], raw_recv.at[h], (side, 0)) for h, cols in enumerate(halves)]
    rank_copy = remote(nrank, rrank, rank_sem.at[0], rank_sem.at[1], (side, 0))

    def row_copies(k):
        pieces = halves if k in relay_to else [slice(0, d_model)]
        return [remote(send.at[rows(k), cols], recv.at[rows(k), cols], row_send.at[0], row_recv.at[k // 2], relay_to.get(k, dests[k]))
                for cols in pieces]

    def gate_copy(k):
        return remote(sgate.at[k], rgate.at[k], gate_sem.at[0], gate_sem.at[1], dests[k])

    final = batches - 2

    def back_copies(k):
        pieces = halves if k // 2 == final else [slice(0, d_model)]
        return [remote(ysend.at[rows(k), cols], yrecv.at[rows(k), cols], back_send.at[0], back_recv.at[batches if h else k // 2], homes[k])
                for h, cols in enumerate(pieces)]

    def wait_rows(i):
        first, count = {0: (1, 1), batches - 1: (partner, 1)}.get(i, (2 * i, 2))
        remote(send.at[rows(first, count), :], recv.at[rows(first, count), :], row_send.at[0], row_recv.at[i], (0, 1)).wait_recv()

    def wait_back(i, cols=slice(0, d_model), sem=None):
        first, count = (partner, 1) if i == batches - 1 else (2 * i, 2)
        remote(ysend.at[rows(first, count), cols], yrecv.at[rows(first, count), cols], back_send.at[0],
               back_recv.at[i if sem is None else sem], (0, 1)).wait_recv()

    for copy in inputs:
        copy.start()
    inputs[2].wait()
    for copy in weights:
        copy.start()
    with scope('barrier'):
        pl.semaphore_wait(barrier, 2)
    tell(known.at[0], (side, 0))
    raw_copies[0].start()

    inputs[0].wait()
    inputs[1].wait()
    ids = ids_ref[...]
    gates = gates_ref[...]
    dev = ids // local
    for k in range(groups):
        chosen[k:k + 1, :] = jnp.max(jnp.where(dev == device(*dests[k]), 1.0, 0.0), axis=0, keepdims=True)
    flags = chosen[...]
    earlier = lax.broadcasted_iota(jnp.int32, (tok_dev, tok_dev), 0) < lax.broadcasted_iota(jnp.int32, (tok_dev, tok_dev), 1)
    order = jnp.dot(flags.astype(bf16), jnp.where(earlier, 1.0, 0.0).astype(bf16), preferred_element_type=f32)
    rank[...] = jnp.where(flags > 0.0, order, -1.0).astype(jnp.int32)
    for i, k in enumerate(near):
        nrank[i:i + 1, :] = rank[k:k + 1, :]
    rank_copy.start()
    with scope('known0'):
        pl.semaphore_wait(known.at[0], 1)
    tell(known.at[1], (-side, 0))

    row_id = lax.broadcasted_iota(jnp.int32, (lanes, tok_dev), 0)
    loc_id = lax.broadcasted_iota(jnp.int32, (local, tok_dev), 0)
    for k in (7, 2, 4, 6, 0, 1, 3, 5):
        onehot = jnp.where(row_id == rank[k:k + 1, :], 1.0, 0.0).astype(bf16)
        pack[rows(k), :] = onehot[:cap, :]
        first = device(*dests[k]) * local
        gate = jnp.zeros((local, tok_dev), f32)
        for j in range(top_k):
            gate += jnp.where(ids[j:j + 1, :] - first == loc_id, gates[j:j + 1, :], 0.0)
        high = gate.astype(bf16).astype(f32)
        mid = (gate - high).astype(bf16).astype(f32)
        low = gate - high - mid
        parts = jnp.concatenate([high, mid, low], axis=0).astype(bf16)
        moved = lax.dot_general(parts, onehot, (((1,), (1,)), ((), ())), preferred_element_type=f32)
        moved = moved[:local] + moved[local:2 * local] + moved[2 * local:]
        if k == own:
            rgate[groups] = moved
        else:
            sgate[k] = moved
    with scope('known1'):
        pl.semaphore_wait(known.at[1], 1)
    tell(known.at[2], (0, 1))
    with scope('known2'):
        pl.semaphore_wait(known.at[2], 1)
    for k in others:
        gate_copy(k).start()
    raw_copies[1].start()
    for k in (partner,) + direct + (own,):
        packed = jnp.dot(pack[rows(k), :], x_ref[...], preferred_element_type=f32).astype(bf16)
        if k == own:
            recv[rows(k), :] = packed
        else:
            send[rows(k), :] = packed
            if k == partner:
                for copy in row_copies(k):
                    copy.start()

    with scope('rankwait'):
        rank_copy.wait_recv()
    for i, k in enumerate(near):
        rpack[i * cap:(i + 1) * cap, :] = jnp.where(row_id[:cap, :] == rrank[i:i + 1, :], 1.0, 0.0).astype(bf16)

    def relay(i, h):
        k, cols = near[i], halves[h]
        packed = jnp.dot(rpack[i * cap:(i + 1) * cap, :], raw[:, cols], preferred_element_type=f32).astype(bf16)
        if k == 0:
            recv[rows(k), cols] = packed
        else:
            send[rows(k), cols] = packed

    with scope('raw0'):
        raw_copies[0].wait_recv()
    with scope('relay0'):
        for i in range(4):
            relay(i, 0)
        for k in (1, 3):
            row_copies(k)[0].start()
    with scope('gates'):
        remote(sgate.at[pl.ds(0, groups - 1)], rgate.at[pl.ds(0, groups - 1)], gate_sem.at[0], gate_sem.at[1], (0, 1)).wait_recv()
        for k in range(groups):
            mine = rgate[groups if k == own else k]
            gcol[k // 2, (k % 2) * cap:(k % 2 + 1) * cap, :] = jnp.concatenate(
                [mine, jnp.zeros((lanes - local, lanes), f32)], axis=0).T[:cap, :]
    with scope('rawsend'):
        raw_copies[0].wait_send()
        raw_copies[1].wait_send()
    for k in direct:
        row_copies(k)[0].start()
    with scope('raw1'):
        raw_copies[1].wait_recv()
    with scope('relay1'):
        for i, k in enumerate(near):
            relay(i, 1)
            if k == 5:
                row_copies(k)[0].start()
            if k > 0:
                row_copies(k)[1].start()

    half = ffn // 2
    third = d_model // 3
    lane_id = lax.broadcasted_iota(jnp.int32, (pair, lanes), 1)

    def hidden(e, base):
        for n in range(2):
            cols = slice(n * half, (n + 1) * half)
            g = jnp.dot(recv[pl.ds(base, pair), :], wg[e, :, cols], preferred_element_type=f32)
            u = jnp.dot(recv[pl.ds(base, pair), :], wu[e, :, cols], preferred_element_type=f32)
            hid[e % 2, :, cols] = (jax.nn.silu(g) * u).astype(bf16)

    def down(e, b, base):
        gate = jnp.sum(jnp.where(lane_id == e, gcol[b], 0.0), axis=1, keepdims=True)
        for n in range(3):
            cols = slice(n * third, (n + 1) * third)
            y = jnp.dot(hid[e % 2], wd[e, :, cols], preferred_element_type=f32).astype(bf16).astype(f32)
            y = jnp.where(gate > 0.0, gate * y, 0.0)
            if e == 0:
                acc[:, cols] = y
            elif e < local - 1:
                acc[:, cols] += y
            else:
                ysend[pl.ds(base, pair), cols] = (acc[:, cols] + y).astype(bf16)

    def batch(b, carry):
        base = pl.multiple_of(b * pair, pair)
        for i in range(batches):
            @pl.when(b == i)
            def _(i=i):
                with scope('rwait%d' % i):
                    wait_rows(i)
        with scope('steps'):
            hidden(0, base)
            for e in range(1, local):
                hidden(e, base)
                down(e - 1, b, base)
            down(local - 1, b, base)
        for i in range(batches):
            @pl.when(b == i)
            def _(i=i):
                if i == own // 2:
                    yrecv[rows(own), :] = ysend[rows(own), :]
                for copies in zip(*[back_copies(k) for k in (2 * i + 1, 2 * i) if k != own]):
                    for copy in copies:
                        copy.start()
        return carry

    with scope('weights'):
        for copy in weights:
            copy.wait()
    lax.fori_loop(0, batches, batch, 0)

    def combine(i, cols):
        span = slice(i * pair, (i + 1) * pair)
        return lax.dot_general(pack[span, :], yrecv[span, cols], (((0,), (0,)), ((), ())), preferred_element_type=f32)

    everything = slice(0, d_model)
    for n, i in enumerate((0, batches - 1, 1)):
        with scope('ywait%d' % i):
            wait_back(i)
        total[...] = (x_ref[...].astype(f32) if n == 0 else total[...]) + combine(i, everything)
    for h, cols in enumerate(halves):
        with scope('yfinal%d' % h):
            wait_back(final, cols, batches if h else final)
        out_ref[:, cols] = (total[:, cols] + combine(final, cols)).astype(bf16)
    with scope('sends'):
        rank_copy.wait_send()
        remote(send.at[pl.ds(0, 6 * cap), :], recv.at[pl.ds(0, 6 * cap), :], row_send.at[0], row_recv.at[0], (0, 1)).wait_send()
        remote(sgate.at[pl.ds(0, groups - 1)], rgate.at[pl.ds(0, groups - 1)], gate_sem.at[0], gate_sem.at[1], (0, 1)).wait_send()
        remote(ysend.at[rows(0, groups - 1), :], yrecv.at[rows(0, groups - 1), :], back_send.at[0], back_recv.at[0], (0, 1)).wait_send()


def solution(mesh):
    groups = mesh.shape['ep']
    row_spec = P(('dp', 'ep'))
    expert_spec = P('ep')

    def device_step(tokens, expert_ids, gate_vals, w_gate, w_up, w_down):
        tok_dev, top_k = expert_ids.shape
        d_model = tokens.shape[1]
        local, _, ffn = w_gate.shape
        cap = tok_dev * (top_k // 2) // groups
        lanes = 128
        f32, bf16 = jnp.float32, jnp.bfloat16
        slots = groups * cap
        dma = pltpu.SemaphoreType.DMA
        return pl.pallas_call(
            functools.partial(moe_kernel, groups, cap),
            out_shape=pltpu.VMEM((tok_dev, d_model), bf16),
            in_specs=[pl.BlockSpec(memory_space=pl.ANY)] * 6,
            out_specs=pl.BlockSpec(memory_space=pltpu.VMEM),
            scratch_shapes=[
                pltpu.VMEM(tokens.shape, bf16),
                pltpu.VMEM((top_k, tok_dev), jnp.int32),
                pltpu.VMEM((top_k, tok_dev), f32),
                pltpu.VMEM(w_gate.shape, bf16),
                pltpu.VMEM(w_up.shape, bf16),
                pltpu.VMEM(w_down.shape, bf16),
                pltpu.VMEM((groups, tok_dev), f32),
                pltpu.VMEM((groups, tok_dev), jnp.int32),
                pltpu.VMEM((groups // 2, tok_dev), jnp.int32),
                pltpu.VMEM((groups // 2, tok_dev), jnp.int32),
                pltpu.VMEM(tokens.shape, bf16),
                pltpu.VMEM((slots // 2, tok_dev), bf16),
                pltpu.VMEM((slots, tok_dev), bf16),
                pltpu.VMEM((slots, d_model), bf16),
                pltpu.VMEM((groups, local, lanes), f32),
                pltpu.VMEM((slots, d_model), bf16),
                pltpu.VMEM((groups + 1, local, lanes), f32),
                pltpu.VMEM((groups // 2, 2 * cap, lanes), f32),
                pltpu.VMEM((2, 2 * cap, ffn), bf16),
                pltpu.VMEM((2 * cap, d_model), f32),
                pltpu.VMEM((slots, d_model), bf16),
                pltpu.VMEM((slots, d_model), bf16),
                pltpu.VMEM((tok_dev, d_model), f32),
                dma((3,)), dma((3,)), dma((2,)), dma((2,)), dma((2,)),
                dma((1,)), dma((groups // 2,)), dma((2,)), dma((1,)), dma((groups // 2 + 1,)), pltpu.SemaphoreType.REGULAR((3,)),
            ],
            compiler_params=pltpu.CompilerParams(collective_id=0, has_side_effects=True, vmem_limit_bytes=56 * 1024 * 1024),
        )(tokens, expert_ids.T, gate_vals.T, w_gate, w_up, w_down)

    return jax.shard_map(device_step, mesh=mesh, in_specs=(row_spec, row_spec, row_spec, expert_spec, expert_spec, expert_spec), out_specs=row_spec, check_vma=False)
```

```python
import contextlib
import functools

import jax
import jax.numpy as jnp
from jax import lax
from jax.experimental import pallas as pl
from jax.experimental.pallas import tpu as pltpu
from jax.sharding import PartitionSpec as P

MESH = pl.DeviceIdType.MESH
CORES = 2


def scope(name):
    return contextlib.nullcontext()


def moe_kernel(groups, cap, x_hbm, ids_hbm, gates_hbm, wg_hbm, wu_hbm, wd_hbm, out_ref,
               x_ref, ids_ref, gates_ref, wg, wu, wd, chosen, rank, nrank, rrank, raw, rpack, pack, send, sgate, recv, rgate,
               gcol, hid, acc, ysend, yrecv, total,
               in_sem, w_sem, raw_send, raw_recv, rank_sem, row_send, row_recv, gate_sem, back_send, back_recv, known):
    tok_dev, d_model = x_ref.shape
    local, _, ffn = wg.shape
    top_k = ids_ref.shape[0]
    lanes = sgate.shape[2]
    chips = groups // CORES
    batches = groups // 2
    pair = 2 * cap
    f32, bf16 = jnp.float32, jnp.bfloat16
    me = lax.axis_index('ep')
    chip, core = me // CORES, me % CORES
    side = 1 - 2 * core
    dests = [(side, 0), (side, 1), (-side, 0), (chips // 2, 0), (-side, 1), (chips // 2, 1), (0, 0), (0, 1)]
    homes = [(-side, 0), (side, 1), (side, 0), (chips // 2, 0), (-side, 1), (chips // 2, 1), (0, 0), (0, 1)]
    direct, near, own, partner = (2, 4), (1, 0, 3, 5), 6, 7
    relay_to = {1: (0, 1), 3: (side, 0), 5: (side, 1)}
    others = [k for k in range(groups) if k != own]

    def device(dx, dc):
        return lax.rem(chip + chips + dx, chips) * CORES + lax.rem(core + dc, CORES)

    def remote(src, dst, send_sem, recv_sem, to):
        return pltpu.make_async_remote_copy(
            src_ref=src, dst_ref=dst, send_sem=send_sem, recv_sem=recv_sem, device_id={'ep': device(*to)}, device_id_type=MESH)

    def rows(k, count=1):
        return pl.ds(k * cap, count * cap)

    def tell(sem, to):
        pl.semaphore_signal(sem, inc=1, device_id={'ep': device(*to)}, device_id_type=MESH)

    barrier = pltpu.get_barrier_semaphore()
    tell(barrier, (-side, 0))
    tell(barrier, (0, 1))

    inputs = [pltpu.make_async_copy(src, dst, in_sem.at[i])
              for i, (src, dst) in enumerate(((ids_hbm, ids_ref), (gates_hbm, gates_ref), (x_hbm, x_ref)))]
    weights = [pltpu.make_async_copy(src, dst, w_sem.at[i])
               for i, (src, dst) in enumerate(((wg_hbm, wg), (wu_hbm, wu), (wd_hbm, wd)))]

    early = d_model // 2
    halves = [slice(0, early), slice(early, d_model)]
    raw_copies = [remote(x_ref.at[:, cols], raw.at[:, cols], raw_send.at[h], raw_recv.at[h], (side, 0)) for h, cols in enumerate(halves)]
    rank_copy = remote(nrank, rrank, rank_sem.at[0], rank_sem.at[1], (side, 0))

    def row_copies(k):
        pieces = halves if k in relay_to else [slice(0, d_model)]
        return [remote(send.at[rows(k), cols], recv.at[rows(k), cols], row_send.at[0], row_recv.at[k // 2], relay_to.get(k, dests[k]))
                for cols in pieces]

    def gate_copy(k):
        return remote(sgate.at[k], rgate.at[k], gate_sem.at[0], gate_sem.at[1], dests[k])

    final = batches - 2

    def back_copies(k):
        pieces = halves if k // 2 == final else [slice(0, d_model)]
        return [remote(ysend.at[rows(k), cols], yrecv.at[rows(k), cols], back_send.at[0], back_recv.at[batches if h else k // 2], homes[k])
                for h, cols in enumerate(pieces)]

    def wait_rows(i):
        first, count = {0: (1, 1), batches - 1: (partner, 1)}.get(i, (2 * i, 2))
        remote(send.at[rows(first, count), :], recv.at[rows(first, count), :], row_send.at[0], row_recv.at[i], (0, 1)).wait_recv()

    def wait_back(i, cols=slice(0, d_model), sem=None):
        first, count = (partner, 1) if i == batches - 1 else (2 * i, 2)
        remote(ysend.at[rows(first, count), cols], yrecv.at[rows(first, count), cols], back_send.at[0],
               back_recv.at[i if sem is None else sem], (0, 1)).wait_recv()

    for copy in inputs:
        copy.start()
    inputs[2].wait()
    for copy in weights:
        copy.start()
    with scope('barrier'):
        pl.semaphore_wait(barrier, 2)
    tell(known.at[0], (side, 0))
    raw_copies[0].start()

    inputs[0].wait()
    inputs[1].wait()
    ids = ids_ref[...]
    gates = gates_ref[...]
    dev = ids // local
    for k in range(groups):
        chosen[k:k + 1, :] = jnp.max(jnp.where(dev == device(*dests[k]), 1.0, 0.0), axis=0, keepdims=True)
    flags = chosen[...]
    earlier = lax.broadcasted_iota(jnp.int32, (tok_dev, tok_dev), 0) < lax.broadcasted_iota(jnp.int32, (tok_dev, tok_dev), 1)
    order = jnp.dot(flags.astype(bf16), jnp.where(earlier, 1.0, 0.0).astype(bf16), preferred_element_type=f32)
    rank[...] = jnp.where(flags > 0.0, order, -1.0).astype(jnp.int32)
    for i, k in enumerate(near):
        nrank[i:i + 1, :] = rank[k:k + 1, :]
    rank_copy.start()
    with scope('known0'):
        pl.semaphore_wait(known.at[0], 1)
    tell(known.at[1], (-side, 0))

    row_id = lax.broadcasted_iota(jnp.int32, (lanes, tok_dev), 0)
    loc_id = lax.broadcasted_iota(jnp.int32, (local, tok_dev), 0)
    expert = lax.broadcasted_iota(jnp.int32, (local, lanes), 0).astype(f32)
    for k in (7, 2, 4, 6, 0, 1, 3, 5):
        onehot = jnp.where(row_id == rank[k:k + 1, :], 1.0, 0.0).astype(bf16)
        pack[rows(k), :] = onehot[:cap, :]
        first = device(*dests[k]) * local
        gate = jnp.zeros((local, tok_dev), f32)
        for j in range(top_k):
            gate += jnp.where(ids[j:j + 1, :] - first == loc_id, gates[j:j + 1, :], 0.0)
        high = gate.astype(bf16).astype(f32)
        mid = (gate - high).astype(bf16).astype(f32)
        low = gate - high - mid
        parts = jnp.concatenate([high, mid, low], axis=0).astype(bf16)
        moved = lax.dot_general(parts, onehot, (((1,), (1,)), ((), ())), preferred_element_type=f32)
        moved = moved[:local] + moved[local:2 * local] + moved[2 * local:]
        low_id = jnp.min(jnp.where(moved > 0.0, expert, float(local)), axis=0, keepdims=True)
        high_id = jnp.max(jnp.where(moved > 0.0, expert, -1.0), axis=0, keepdims=True)
        moved = jnp.concatenate([jnp.sum(jnp.where(expert == low_id, moved, 0.0), axis=0, keepdims=True),
                                 jnp.sum(jnp.where(expert == high_id, moved, 0.0), axis=0, keepdims=True), low_id, high_id], axis=0)
        if k == own:
            rgate[groups] = moved
        else:
            sgate[k] = moved
    with scope('known1'):
        pl.semaphore_wait(known.at[1], 1)
    tell(known.at[2], (0, 1))
    with scope('known2'):
        pl.semaphore_wait(known.at[2], 1)
    for k in others:
        gate_copy(k).start()
    raw_copies[1].start()
    for k in (partner,) + direct + (own,):
        packed = jnp.dot(pack[rows(k), :], x_ref[...], preferred_element_type=f32).astype(bf16)
        if k == own:
            recv[rows(k), :] = packed
        else:
            send[rows(k), :] = packed
            if k == partner:
                for copy in row_copies(k):
                    copy.start()

    with scope('rankwait'):
        rank_copy.wait_recv()
    for i, k in enumerate(near):
        rpack[i * cap:(i + 1) * cap, :] = jnp.where(row_id[:cap, :] == rrank[i:i + 1, :], 1.0, 0.0).astype(bf16)

    def relay(i, h):
        k, cols = near[i], halves[h]
        packed = jnp.dot(rpack[i * cap:(i + 1) * cap, :], raw[:, cols], preferred_element_type=f32).astype(bf16)
        if k == 0:
            recv[rows(k), cols] = packed
        else:
            send[rows(k), cols] = packed

    with scope('raw0'):
        raw_copies[0].wait_recv()
    with scope('relay0'):
        for i in range(4):
            relay(i, 0)
        for k in (1, 3):
            row_copies(k)[0].start()
    with scope('gates'):
        remote(sgate.at[pl.ds(0, groups - 1)], rgate.at[pl.ds(0, groups - 1)], gate_sem.at[0], gate_sem.at[1], (0, 1)).wait_recv()
        for k in range(groups):
            two = rgate[groups if k == own else k]
            mine = jnp.where(expert == two[2:3], two[0:1], jnp.where(expert == two[3:4], two[1:2], 0.0))
            gcol[k // 2, (k % 2) * cap:(k % 2 + 1) * cap, :] = jnp.concatenate(
                [mine, jnp.zeros((lanes - local, lanes), f32)], axis=0).T[:cap, :]
    with scope('rawsend'):
        raw_copies[0].wait_send()
        raw_copies[1].wait_send()
    for k in direct:
        row_copies(k)[0].start()
    with scope('raw1'):
        raw_copies[1].wait_recv()
    with scope('relay1'):
        for i, k in enumerate(near):
            relay(i, 1)
            if k == 5:
                row_copies(k)[0].start()
            if k > 0:
                row_copies(k)[1].start()

    half = ffn // 2
    third = d_model // 3
    lane_id = lax.broadcasted_iota(jnp.int32, (pair, lanes), 1)

    def hidden(e, base):
        for n in range(2):
            cols = slice(n * half, (n + 1) * half)
            g = jnp.dot(recv[pl.ds(base, pair), :], wg[e, :, cols], preferred_element_type=f32)
            u = jnp.dot(recv[pl.ds(base, pair), :], wu[e, :, cols], preferred_element_type=f32)
            hid[e % 2, :, cols] = (jax.nn.silu(g) * u).astype(bf16)

    def down(e, b, base):
        gate = jnp.sum(jnp.where(lane_id == e, gcol[b], 0.0), axis=1, keepdims=True)
        for n in range(3):
            cols = slice(n * third, (n + 1) * third)
            y = jnp.dot(hid[e % 2], wd[e, :, cols], preferred_element_type=f32).astype(bf16).astype(f32)
            y = jnp.where(gate > 0.0, gate * y, 0.0)
            if e == 0:
                acc[:, cols] = y
            elif e < local - 1:
                acc[:, cols] += y
            else:
                ysend[pl.ds(base, pair), cols] = (acc[:, cols] + y).astype(bf16)

    def batch(b, carry):
        base = pl.multiple_of(b * pair, pair)
        for i in range(batches):
            @pl.when(b == i)
            def _(i=i):
                with scope('rwait%d' % i):
                    wait_rows(i)
        with scope('steps'):
            hidden(0, base)
            for e in range(1, local):
                hidden(e, base)
                down(e - 1, b, base)
            down(local - 1, b, base)
        for i in range(batches):
            @pl.when(b == i)
            def _(i=i):
                if i == own // 2:
                    yrecv[rows(own), :] = ysend[rows(own), :]
                for copies in zip(*[back_copies(k) for k in (2 * i + 1, 2 * i) if k != own]):
                    for copy in copies:
                        copy.start()
        return carry

    with scope('weights'):
        for copy in weights:
            copy.wait()
    lax.fori_loop(0, batches, batch, 0)

    def combine(i, cols):
        span = slice(i * pair, (i + 1) * pair)
        return lax.dot_general(pack[span, :], yrecv[span, cols], (((0,), (0,)), ((), ())), preferred_element_type=f32)

    everything = slice(0, d_model)
    for n, i in enumerate((0, batches - 1, 1)):
        with scope('ywait%d' % i):
            wait_back(i)
        total[...] = (x_ref[...].astype(f32) if n == 0 else total[...]) + combine(i, everything)
    for h, cols in enumerate(halves):
        with scope('yfinal%d' % h):
            wait_back(final, cols, batches if h else final)
        out_ref[:, cols] = (total[:, cols] + combine(final, cols)).astype(bf16)
    with scope('sends'):
        rank_copy.wait_send()
        remote(send.at[pl.ds(0, 6 * cap), :], recv.at[pl.ds(0, 6 * cap), :], row_send.at[0], row_recv.at[0], (0, 1)).wait_send()
        remote(sgate.at[pl.ds(0, groups - 1)], rgate.at[pl.ds(0, groups - 1)], gate_sem.at[0], gate_sem.at[1], (0, 1)).wait_send()
        remote(ysend.at[rows(0, groups - 1), :], yrecv.at[rows(0, groups - 1), :], back_send.at[0], back_recv.at[0], (0, 1)).wait_send()


def solution(mesh):
    groups = mesh.shape['ep']
    row_spec = P(('dp', 'ep'))
    expert_spec = P('ep')

    def device_step(tokens, expert_ids, gate_vals, w_gate, w_up, w_down):
        tok_dev, top_k = expert_ids.shape
        d_model = tokens.shape[1]
        local, _, ffn = w_gate.shape
        cap = tok_dev * (top_k // 2) // groups
        lanes = 128
        f32, bf16 = jnp.float32, jnp.bfloat16
        slots = groups * cap
        dma = pltpu.SemaphoreType.DMA
        return pl.pallas_call(
            functools.partial(moe_kernel, groups, cap),
            out_shape=pltpu.VMEM((tok_dev, d_model), bf16),
            in_specs=[pl.BlockSpec(memory_space=pl.ANY)] * 6,
            out_specs=pl.BlockSpec(memory_space=pltpu.VMEM),
            scratch_shapes=[
                pltpu.VMEM(tokens.shape, bf16),
                pltpu.VMEM((top_k, tok_dev), jnp.int32),
                pltpu.VMEM((top_k, tok_dev), f32),
                pltpu.VMEM(w_gate.shape, bf16),
                pltpu.VMEM(w_up.shape, bf16),
                pltpu.VMEM(w_down.shape, bf16),
                pltpu.VMEM((groups, tok_dev), f32),
                pltpu.VMEM((groups, tok_dev), jnp.int32),
                pltpu.VMEM((groups // 2, tok_dev), jnp.int32),
                pltpu.VMEM((groups // 2, tok_dev), jnp.int32),
                pltpu.VMEM(tokens.shape, bf16),
                pltpu.VMEM((slots // 2, tok_dev), bf16),
                pltpu.VMEM((slots, tok_dev), bf16),
                pltpu.VMEM((slots, d_model), bf16),
                pltpu.VMEM((groups, 4, lanes), f32),
                pltpu.VMEM((slots, d_model), bf16),
                pltpu.VMEM((groups + 1, 4, lanes), f32),
                pltpu.VMEM((groups // 2, 2 * cap, lanes), f32),
                pltpu.VMEM((2, 2 * cap, ffn), bf16),
                pltpu.VMEM((2 * cap, d_model), f32),
                pltpu.VMEM((slots, d_model), bf16),
                pltpu.VMEM((slots, d_model), bf16),
                pltpu.VMEM((tok_dev, d_model), f32),
                dma((3,)), dma((3,)), dma((2,)), dma((2,)), dma((2,)),
                dma((1,)), dma((groups // 2,)), dma((2,)), dma((1,)), dma((groups // 2 + 1,)), pltpu.SemaphoreType.REGULAR((3,)),
            ],
            compiler_params=pltpu.CompilerParams(collective_id=0, has_side_effects=True, vmem_limit_bytes=56 * 1024 * 1024),
        )(tokens, expert_ids.T, gate_vals.T, w_gate, w_up, w_down)

    return jax.shard_map(device_step, mesh=mesh, in_specs=(row_spec, row_spec, row_spec, expert_spec, expert_spec, expert_spec), out_specs=row_spec, check_vma=False)
```

```python
import contextlib
import functools

import jax
import jax.numpy as jnp
from jax import lax
from jax.experimental import pallas as pl
from jax.experimental.pallas import tpu as pltpu
from jax.sharding import PartitionSpec as P

MESH = pl.DeviceIdType.MESH
CORES = 2


def scope(name):
    return contextlib.nullcontext()


def moe_kernel(groups, cap, x_hbm, ids_hbm, gates_hbm, wg_hbm, wu_hbm, wd_hbm, out_ref,
               x_ref, ids_ref, gates_ref, wg, wu, wd, chosen, rank, nrank, rrank, raw, rpack, pack, send, sgate, recv, rgate,
               gcol, hid, acc, ysend, yrecv, total,
               in_sem, w_sem, raw_send, raw_recv, rank_sem, row_send, row_recv, gate_sem, back_send, back_recv, known):
    tok_dev, d_model = x_ref.shape
    local, _, ffn = wg.shape
    top_k = ids_ref.shape[0]
    lanes = sgate.shape[2]
    chips = groups // CORES
    batches = groups // 2
    pair = 2 * cap
    f32, bf16 = jnp.float32, jnp.bfloat16
    me = lax.axis_index('ep')
    chip, core = me // CORES, me % CORES
    side = 1 - 2 * core
    dests = [(side, 0), (side, 1), (-side, 0), (chips // 2, 0), (-side, 1), (chips // 2, 1), (0, 0), (0, 1)]
    homes = [(-side, 0), (side, 1), (side, 0), (chips // 2, 0), (-side, 1), (chips // 2, 1), (0, 0), (0, 1)]
    direct, near, own, partner = (2, 4), (1, 0, 3, 5), 6, 7
    relay_to = {1: (0, 1), 3: (side, 0), 5: (side, 1)}
    others = [k for k in range(groups) if k != own]

    def device(dx, dc):
        return lax.rem(chip + chips + dx, chips) * CORES + lax.rem(core + dc, CORES)

    def remote(src, dst, send_sem, recv_sem, to):
        return pltpu.make_async_remote_copy(
            src_ref=src, dst_ref=dst, send_sem=send_sem, recv_sem=recv_sem, device_id={'ep': device(*to)}, device_id_type=MESH)

    def rows(k, count=1):
        return pl.ds(k * cap, count * cap)

    def tell(sem, to):
        pl.semaphore_signal(sem, inc=1, device_id={'ep': device(*to)}, device_id_type=MESH)

    barrier = pltpu.get_barrier_semaphore()
    tell(barrier, (-side, 0))
    tell(barrier, (0, 1))

    inputs = [pltpu.make_async_copy(src, dst, in_sem.at[i])
              for i, (src, dst) in enumerate(((ids_hbm, ids_ref), (gates_hbm, gates_ref), (x_hbm, x_ref)))]
    weights = [pltpu.make_async_copy(src, dst, w_sem.at[i])
               for i, (src, dst) in enumerate(((wg_hbm, wg), (wu_hbm, wu), (wd_hbm, wd)))]

    early = d_model * 2 // 3
    halves = [slice(0, early), slice(early, d_model)]
    raw_copies = [remote(x_ref.at[:, cols], raw.at[:, cols], raw_send.at[h], raw_recv.at[h], (side, 0)) for h, cols in enumerate(halves)]
    rank_copy = remote(nrank, rrank, rank_sem.at[0], rank_sem.at[1], (side, 0))

    def row_copies(k):
        pieces = halves if k in relay_to else [slice(0, d_model)]
        return [remote(send.at[rows(k), cols], recv.at[rows(k), cols], row_send.at[0], row_recv.at[k // 2], relay_to.get(k, dests[k]))
                for cols in pieces]

    def gate_copy(k):
        return remote(sgate.at[k], rgate.at[k], gate_sem.at[0], gate_sem.at[1], dests[k])

    final = batches - 2

    def back_copies(k):
        pieces = halves if k // 2 == final else [slice(0, d_model)]
        return [remote(ysend.at[rows(k), cols], yrecv.at[rows(k), cols], back_send.at[0], back_recv.at[batches if h else k // 2], homes[k])
                for h, cols in enumerate(pieces)]

    def wait_rows(i):
        first, count = {0: (1, 1), batches - 1: (partner, 1)}.get(i, (2 * i, 2))
        remote(send.at[rows(first, count), :], recv.at[rows(first, count), :], row_send.at[0], row_recv.at[i], (0, 1)).wait_recv()

    def wait_back(i, cols=slice(0, d_model), sem=None):
        first, count = (partner, 1) if i == batches - 1 else (2 * i, 2)
        remote(ysend.at[rows(first, count), cols], yrecv.at[rows(first, count), cols], back_send.at[0],
               back_recv.at[i if sem is None else sem], (0, 1)).wait_recv()

    for copy in inputs:
        copy.start()
    inputs[2].wait()
    for copy in weights:
        copy.start()
    with scope('barrier'):
        pl.semaphore_wait(barrier, 2)
    tell(known.at[0], (side, 0))
    raw_copies[0].start()

    inputs[0].wait()
    inputs[1].wait()
    ids = ids_ref[...]
    gates = gates_ref[...]
    dev = ids // local
    for k in range(groups):
        chosen[k:k + 1, :] = jnp.max(jnp.where(dev == device(*dests[k]), 1.0, 0.0), axis=0, keepdims=True)
    flags = chosen[...]
    earlier = lax.broadcasted_iota(jnp.int32, (tok_dev, tok_dev), 0) < lax.broadcasted_iota(jnp.int32, (tok_dev, tok_dev), 1)
    order = jnp.dot(flags.astype(bf16), jnp.where(earlier, 1.0, 0.0).astype(bf16), preferred_element_type=f32)
    rank[...] = jnp.where(flags > 0.0, order, -1.0).astype(jnp.int32)
    for i, k in enumerate(near):
        nrank[i:i + 1, :] = rank[k:k + 1, :]
    rank_copy.start()
    with scope('known0'):
        pl.semaphore_wait(known.at[0], 1)
    tell(known.at[1], (-side, 0))

    row_id = lax.broadcasted_iota(jnp.int32, (lanes, tok_dev), 0)
    loc_id = lax.broadcasted_iota(jnp.int32, (local, tok_dev), 0)
    expert = lax.broadcasted_iota(jnp.int32, (local, lanes), 0).astype(f32)
    for k in (7, 2, 4, 6, 0, 1, 3, 5):
        onehot = jnp.where(row_id == rank[k:k + 1, :], 1.0, 0.0).astype(bf16)
        pack[rows(k), :] = onehot[:cap, :]
        first = device(*dests[k]) * local
        gate = jnp.zeros((local, tok_dev), f32)
        for j in range(top_k):
            gate += jnp.where(ids[j:j + 1, :] - first == loc_id, gates[j:j + 1, :], 0.0)
        high = jnp.minimum(gate, float(jnp.finfo(bf16).max)).astype(bf16).astype(f32)
        mid = (gate - high).astype(bf16).astype(f32)
        low = gate - high - mid
        parts = jnp.concatenate([high, mid, low], axis=0).astype(bf16)
        moved = lax.dot_general(parts, onehot, (((1,), (1,)), ((), ())), preferred_element_type=f32)
        moved = moved[:local] + moved[local:2 * local] + moved[2 * local:]
        low_id = jnp.min(jnp.where(moved > 0.0, expert, float(local)), axis=0, keepdims=True)
        high_id = jnp.max(jnp.where(moved > 0.0, expert, -1.0), axis=0, keepdims=True)
        moved = jnp.concatenate([jnp.sum(jnp.where(expert == low_id, moved, 0.0), axis=0, keepdims=True),
                                 jnp.sum(jnp.where(expert == high_id, moved, 0.0), axis=0, keepdims=True), low_id, high_id], axis=0)
        if k == own:
            rgate[groups] = moved
        else:
            sgate[k] = moved
    with scope('known1'):
        pl.semaphore_wait(known.at[1], 1)
    tell(known.at[2], (0, 1))
    with scope('known2'):
        pl.semaphore_wait(known.at[2], 1)
    for k in others:
        gate_copy(k).start()
    raw_copies[1].start()
    for k in (partner,) + direct + (own,):
        packed = jnp.dot(pack[rows(k), :], x_ref[...], preferred_element_type=f32).astype(bf16)
        if k == own:
            recv[rows(k), :] = packed
        else:
            send[rows(k), :] = packed
            if k == partner:
                for copy in row_copies(k):
                    copy.start()

    with scope('rankwait'):
        rank_copy.wait_recv()
    for i, k in enumerate(near):
        rpack[i * cap:(i + 1) * cap, :] = jnp.where(row_id[:cap, :] == rrank[i:i + 1, :], 1.0, 0.0).astype(bf16)

    def relay(i, h):
        k, cols = near[i], halves[h]
        packed = jnp.dot(rpack[i * cap:(i + 1) * cap, :], raw[:, cols], preferred_element_type=f32).astype(bf16)
        if k == 0:
            recv[rows(k), cols] = packed
        else:
            send[rows(k), cols] = packed

    with scope('raw0'):
        raw_copies[0].wait_recv()
    with scope('relay0'):
        for i in range(4):
            relay(i, 0)
        for k in (1, 3):
            row_copies(k)[0].start()
    with scope('gates'):
        remote(sgate.at[pl.ds(0, groups - 1)], rgate.at[pl.ds(0, groups - 1)], gate_sem.at[0], gate_sem.at[1], (0, 1)).wait_recv()
        for k in range(groups):
            two = rgate[groups if k == own else k]
            mine = jnp.where(expert == two[2:3], two[0:1], jnp.where(expert == two[3:4], two[1:2], 0.0))
            gcol[k // 2, (k % 2) * cap:(k % 2 + 1) * cap, :] = jnp.concatenate(
                [mine, jnp.zeros((lanes - local, lanes), f32)], axis=0).T[:cap, :]
    with scope('rawsend'):
        raw_copies[0].wait_send()
        raw_copies[1].wait_send()
    for k in direct:
        row_copies(k)[0].start()
    with scope('raw1'):
        raw_copies[1].wait_recv()
    with scope('relay1'):
        for i, k in enumerate(near):
            relay(i, 1)
            if k == 5:
                row_copies(k)[0].start()
            if k > 0:
                row_copies(k)[1].start()

    half = ffn // 2
    third = d_model // 3
    lane_id = lax.broadcasted_iota(jnp.int32, (pair, lanes), 1)

    def hidden(e, base):
        for n in range(2):
            cols = slice(n * half, (n + 1) * half)
            g = jnp.dot(recv[pl.ds(base, pair), :], wg[e, :, cols], preferred_element_type=f32)
            u = jnp.dot(recv[pl.ds(base, pair), :], wu[e, :, cols], preferred_element_type=f32)
            hid[e % 2, :, cols] = (jax.nn.silu(g) * u).astype(bf16)

    def down(e, b, base):
        gate = jnp.sum(jnp.where(lane_id == e, gcol[b], 0.0), axis=1, keepdims=True)
        for n in range(3):
            cols = slice(n * third, (n + 1) * third)
            y = jnp.dot(hid[e % 2], wd[e, :, cols], preferred_element_type=f32).astype(bf16).astype(f32)
            y = jnp.where(gate > 0.0, gate * y, 0.0)
            if e == 0:
                acc[:, cols] = y
            elif e < local - 1:
                acc[:, cols] += y
            else:
                ysend[pl.ds(base, pair), cols] = (acc[:, cols] + y).astype(bf16)

    def batch(b, carry):
        base = pl.multiple_of(b * pair, pair)
        for i in range(batches):
            @pl.when(b == i)
            def _(i=i):
                with scope('rwait%d' % i):
                    wait_rows(i)
        with scope('steps'):
            hidden(0, base)
            for e in range(1, local):
                hidden(e, base)
                down(e - 1, b, base)
            down(local - 1, b, base)
        for i in range(batches):
            @pl.when(b == i)
            def _(i=i):
                if i == own // 2:
                    yrecv[rows(own), :] = ysend[rows(own), :]
                for copies in zip(*[back_copies(k) for k in (2 * i + 1, 2 * i) if k != own]):
                    for copy in copies:
                        copy.start()
        return carry

    with scope('weights'):
        for copy in weights:
            copy.wait()
    lax.fori_loop(0, batches, batch, 0)

    def combine(i, cols):
        span = slice(i * pair, (i + 1) * pair)
        return lax.dot_general(pack[span, :], yrecv[span, cols], (((0,), (0,)), ((), ())), preferred_element_type=f32)

    everything = slice(0, d_model)
    for n, i in enumerate((0, batches - 1, 1)):
        with scope('ywait%d' % i):
            wait_back(i)
        total[...] = (x_ref[...].astype(f32) if n == 0 else total[...]) + combine(i, everything)
    for h, cols in enumerate(halves):
        with scope('yfinal%d' % h):
            wait_back(final, cols, batches if h else final)
        out_ref[:, cols] = (total[:, cols] + combine(final, cols)).astype(bf16)
    with scope('sends'):
        rank_copy.wait_send()
        remote(send.at[pl.ds(0, 6 * cap), :], recv.at[pl.ds(0, 6 * cap), :], row_send.at[0], row_recv.at[0], (0, 1)).wait_send()
        remote(sgate.at[pl.ds(0, groups - 1)], rgate.at[pl.ds(0, groups - 1)], gate_sem.at[0], gate_sem.at[1], (0, 1)).wait_send()
        remote(ysend.at[rows(0, groups - 1), :], yrecv.at[rows(0, groups - 1), :], back_send.at[0], back_recv.at[0], (0, 1)).wait_send()


def solution(mesh):
    groups = mesh.shape['ep']
    row_spec = P(('dp', 'ep'))
    expert_spec = P('ep')

    def device_step(tokens, expert_ids, gate_vals, w_gate, w_up, w_down):
        tok_dev, top_k = expert_ids.shape
        d_model = tokens.shape[1]
        local, _, ffn = w_gate.shape
        cap = tok_dev * (top_k // 2) // groups
        lanes = 128
        f32, bf16 = jnp.float32, jnp.bfloat16
        slots = groups * cap
        dma = pltpu.SemaphoreType.DMA
        return pl.pallas_call(
            functools.partial(moe_kernel, groups, cap),
            out_shape=pltpu.VMEM((tok_dev, d_model), bf16),
            in_specs=[pl.BlockSpec(memory_space=pl.ANY)] * 6,
            out_specs=pl.BlockSpec(memory_space=pltpu.VMEM),
            scratch_shapes=[
                pltpu.VMEM(tokens.shape, bf16),
                pltpu.VMEM((top_k, tok_dev), jnp.int32),
                pltpu.VMEM((top_k, tok_dev), f32),
                pltpu.VMEM(w_gate.shape, bf16),
                pltpu.VMEM(w_up.shape, bf16),
                pltpu.VMEM(w_down.shape, bf16),
                pltpu.VMEM((groups, tok_dev), f32),
                pltpu.VMEM((groups, tok_dev), jnp.int32),
                pltpu.VMEM((groups // 2, tok_dev), jnp.int32),
                pltpu.VMEM((groups // 2, tok_dev), jnp.int32),
                pltpu.VMEM(tokens.shape, bf16),
                pltpu.VMEM((slots // 2, tok_dev), bf16),
                pltpu.VMEM((slots, tok_dev), bf16),
                pltpu.VMEM((slots, d_model), bf16),
                pltpu.VMEM((groups, 4, lanes), f32),
                pltpu.VMEM((slots, d_model), bf16),
                pltpu.VMEM((groups + 1, 4, lanes), f32),
                pltpu.VMEM((groups // 2, 2 * cap, lanes), f32),
                pltpu.VMEM((2, 2 * cap, ffn), bf16),
                pltpu.VMEM((2 * cap, d_model), f32),
                pltpu.VMEM((slots, d_model), bf16),
                pltpu.VMEM((slots, d_model), bf16),
                pltpu.VMEM((tok_dev, d_model), f32),
                dma((3,)), dma((3,)), dma((2,)), dma((2,)), dma((2,)),
                dma((1,)), dma((groups // 2,)), dma((2,)), dma((1,)), dma((groups // 2 + 1,)), pltpu.SemaphoreType.REGULAR((3,)),
            ],
            compiler_params=pltpu.CompilerParams(collective_id=0, has_side_effects=True, vmem_limit_bytes=56 * 1024 * 1024),
        )(tokens, expert_ids.T, gate_vals.T, w_gate, w_up, w_down)

    return jax.shard_map(device_step, mesh=mesh, in_specs=(row_spec, row_spec, row_spec, expert_spec, expert_spec, expert_spec), out_specs=row_spec, check_vma=False)
```

```python
import contextlib
import functools

import jax
import jax.numpy as jnp
from jax import lax
from jax.experimental import pallas as pl
from jax.experimental.pallas import tpu as pltpu
from jax.sharding import PartitionSpec as P

MESH = pl.DeviceIdType.MESH
CORES = 2


def scope(name):
    return contextlib.nullcontext()


def moe_kernel(groups, cap, x_hbm, ids_hbm, gates_hbm, wg_hbm, wu_hbm, wd_hbm, out_ref,
               x_ref, ids_ref, gates_ref, wg, wu, wd, chosen, rank, nrank, rrank, raw, rpack, pack, send, sgate, recv, rgate,
               gcol, hid, acc, ysend, yrecv, total,
               in_sem, w_sem, raw_send, raw_recv, rank_sem, row_send, row_recv, gate_sem, back_send, back_recv, known):
    tok_dev, d_model = x_ref.shape
    local, _, ffn = wg.shape
    top_k = ids_ref.shape[0]
    lanes = sgate.shape[2]
    chips = groups // CORES
    batches = groups // 2
    pair = 2 * cap
    f32, bf16 = jnp.float32, jnp.bfloat16
    me = lax.axis_index('ep')
    chip, core = me // CORES, me % CORES
    side = 1 - 2 * core
    dests = [(side, 0), (side, 1), (-side, 0), (chips // 2, 0), (-side, 1), (chips // 2, 1), (0, 0), (0, 1)]
    homes = [(-side, 0), (side, 1), (side, 0), (chips // 2, 0), (-side, 1), (chips // 2, 1), (0, 0), (0, 1)]
    direct, near, own, partner = (2, 4), (1, 0, 3, 5), 6, 7
    relay_to = {1: (0, 1), 3: (side, 0), 5: (side, 1)}
    others = [k for k in range(groups) if k != own]

    def device(dx, dc):
        return lax.rem(chip + chips + dx, chips) * CORES + lax.rem(core + dc, CORES)

    def remote(src, dst, send_sem, recv_sem, to):
        return pltpu.make_async_remote_copy(
            src_ref=src, dst_ref=dst, send_sem=send_sem, recv_sem=recv_sem, device_id={'ep': device(*to)}, device_id_type=MESH)

    def rows(k, count=1):
        return pl.ds(k * cap, count * cap)

    def tell(sem, to):
        pl.semaphore_signal(sem, inc=1, device_id={'ep': device(*to)}, device_id_type=MESH)

    barrier = pltpu.get_barrier_semaphore()
    tell(barrier, (-side, 0))
    tell(barrier, (0, 1))

    inputs = [pltpu.make_async_copy(src, dst, in_sem.at[i])
              for i, (src, dst) in enumerate(((ids_hbm, ids_ref), (gates_hbm, gates_ref), (x_hbm, x_ref)))]
    weights = [pltpu.make_async_copy(src, dst, w_sem.at[i])
               for i, (src, dst) in enumerate(((wg_hbm, wg), (wu_hbm, wu), (wd_hbm, wd)))]

    early = d_model * 2 // 3
    halves = [slice(0, early), slice(early, d_model)]
    raw_copies = [remote(x_ref.at[:, cols], raw.at[:, cols], raw_send.at[0], raw_recv.at[h], (side, 0)) for h, cols in enumerate(halves)]
    rank_copy = remote(nrank, rrank, rank_sem.at[0], rank_sem.at[1], (side, 0))

    def row_copies(k):
        pieces = halves if k in relay_to else [slice(0, d_model)]
        return [remote(send.at[rows(k), cols], recv.at[rows(k), cols], row_send.at[0], row_recv.at[k // 2], relay_to.get(k, dests[k]))
                for cols in pieces]

    def gate_copy(k):
        return remote(sgate.at[k], rgate.at[k], gate_sem.at[0], gate_sem.at[1], dests[k])

    final = batches - 2

    def back_copies(k):
        pieces = halves if k // 2 == final else [slice(0, d_model)]
        return [remote(ysend.at[rows(k), cols], yrecv.at[rows(k), cols], back_send.at[0], back_recv.at[0 if k // 2 != final else 1 + h], homes[k])
                for h, cols in enumerate(pieces)]

    def wait_rows(i):
        first, count = {0: (1, 1), batches - 1: (partner, 1)}.get(i, (2 * i, 2))
        remote(send.at[rows(first, count), :], recv.at[rows(first, count), :], row_send.at[0], row_recv.at[i], (0, 1)).wait_recv()

    def wait_back(first, count, cols, sem):
        remote(ysend.at[rows(first, count), cols], yrecv.at[rows(first, count), cols], back_send.at[0], back_recv.at[sem], (0, 1)).wait_recv()

    for copy in inputs:
        copy.start()
    inputs[2].wait()
    for copy in weights:
        copy.start()
    with scope('barrier'):
        pl.semaphore_wait(barrier, 2)
    tell(known.at[0], (side, 0))
    raw_copies[0].start()

    inputs[0].wait()
    inputs[1].wait()
    ids = ids_ref[...]
    gates = gates_ref[...]
    dev = ids // local
    for k in range(groups):
        chosen[k:k + 1, :] = jnp.max(jnp.where(dev == device(*dests[k]), 1.0, 0.0), axis=0, keepdims=True)
    flags = chosen[...]
    earlier = lax.broadcasted_iota(jnp.int32, (tok_dev, tok_dev), 0) < lax.broadcasted_iota(jnp.int32, (tok_dev, tok_dev), 1)
    order = jnp.dot(flags.astype(bf16), jnp.where(earlier, 1.0, 0.0).astype(bf16), preferred_element_type=f32)
    rank[...] = jnp.where(flags > 0.0, order, -1.0).astype(jnp.int32)
    for i, k in enumerate(near):
        nrank[i:i + 1, :] = rank[k:k + 1, :]
    rank_copy.start()
    with scope('known0'):
        pl.semaphore_wait(known.at[0], 1)
    tell(known.at[1], (-side, 0))

    row_id = lax.broadcasted_iota(jnp.int32, (lanes, tok_dev), 0)
    loc_id = lax.broadcasted_iota(jnp.int32, (local, tok_dev), 0)
    expert = lax.broadcasted_iota(jnp.int32, (local, lanes), 0).astype(f32)
    for k in (7, 2, 4, 6, 0, 1, 3, 5):
        onehot = jnp.where(row_id == rank[k:k + 1, :], 1.0, 0.0).astype(bf16)
        pack[rows(k), :] = onehot[:cap, :]
        first = device(*dests[k]) * local
        gate = jnp.zeros((local, tok_dev), f32)
        for j in range(top_k):
            gate += jnp.where(ids[j:j + 1, :] - first == loc_id, gates[j:j + 1, :], 0.0)
        high = jnp.minimum(gate, float(jnp.finfo(bf16).max)).astype(bf16).astype(f32)
        mid = (gate - high).astype(bf16).astype(f32)
        low = gate - high - mid
        parts = jnp.concatenate([high, mid, low], axis=0).astype(bf16)
        moved = lax.dot_general(parts, onehot, (((1,), (1,)), ((), ())), preferred_element_type=f32)
        moved = moved[:local] + moved[local:2 * local] + moved[2 * local:]
        low_id = jnp.min(jnp.where(moved > 0.0, expert, float(local)), axis=0, keepdims=True)
        high_id = jnp.max(jnp.where(moved > 0.0, expert, -1.0), axis=0, keepdims=True)
        moved = jnp.concatenate([jnp.sum(jnp.where(expert == low_id, moved, 0.0), axis=0, keepdims=True),
                                 jnp.sum(jnp.where(expert == high_id, moved, 0.0), axis=0, keepdims=True), low_id, high_id], axis=0)
        if k == own:
            rgate[groups] = moved
        else:
            sgate[k] = moved
    with scope('known1'):
        pl.semaphore_wait(known.at[1], 1)
    tell(known.at[2], (0, 1))
    with scope('known2'):
        pl.semaphore_wait(known.at[2], 1)
    for k in others:
        gate_copy(k).start()
    raw_copies[1].start()
    for k in (partner,) + direct + (own,):
        packed = jnp.dot(pack[rows(k), :], x_ref[...], preferred_element_type=f32).astype(bf16)
        if k == own:
            recv[rows(k), :] = packed
        else:
            send[rows(k), :] = packed
            if k == partner:
                for copy in row_copies(k):
                    copy.start()

    with scope('rankwait'):
        rank_copy.wait_recv()
    for i, k in enumerate(near):
        rpack[i * cap:(i + 1) * cap, :] = jnp.where(row_id[:cap, :] == rrank[i:i + 1, :], 1.0, 0.0).astype(bf16)

    def relay(i, h):
        k, cols = near[i], halves[h]
        packed = jnp.dot(rpack[i * cap:(i + 1) * cap, :], raw[:, cols], preferred_element_type=f32).astype(bf16)
        if k == 0:
            recv[rows(k), cols] = packed
        else:
            send[rows(k), cols] = packed

    with scope('raw0'):
        raw_copies[0].wait_recv()
    with scope('relay0'):
        for i in range(4):
            relay(i, 0)
        for k in (1, 3):
            row_copies(k)[0].start()
    with scope('gates'):
        remote(sgate.at[pl.ds(0, groups - 1)], rgate.at[pl.ds(0, groups - 1)], gate_sem.at[0], gate_sem.at[1], (0, 1)).wait_recv()
        for k in range(groups):
            two = rgate[groups if k == own else k]
            mine = jnp.where(expert == two[2:3], two[0:1], jnp.where(expert == two[3:4], two[1:2], 0.0))
            gcol[k // 2, (k % 2) * cap:(k % 2 + 1) * cap, :] = jnp.concatenate(
                [mine, jnp.zeros((lanes - local, lanes), f32)], axis=0).T[:cap, :]
    with scope('rawsend'):
        remote(x_ref, raw, raw_send.at[0], raw_recv.at[0], (side, 0)).wait_send()
    for k in direct:
        row_copies(k)[0].start()
    with scope('raw1'):
        raw_copies[1].wait_recv()
    with scope('relay1'):
        for i, k in enumerate(near):
            relay(i, 1)
            if k == 5:
                row_copies(k)[0].start()
            if k > 0:
                row_copies(k)[1].start()

    half = ffn // 2
    third = d_model // 3
    lane_id = lax.broadcasted_iota(jnp.int32, (pair, lanes), 1)

    def hidden(e, base):
        for n in range(2):
            cols = slice(n * half, (n + 1) * half)
            g = jnp.dot(recv[pl.ds(base, pair), :], wg[e, :, cols], preferred_element_type=f32)
            u = jnp.dot(recv[pl.ds(base, pair), :], wu[e, :, cols], preferred_element_type=f32)
            hid[e % 2, :, cols] = (jax.nn.silu(g) * u).astype(bf16)

    def down(e, b, base):
        gate = jnp.sum(jnp.where(lane_id == e, gcol[b], 0.0), axis=1, keepdims=True)
        for n in range(3):
            cols = slice(n * third, (n + 1) * third)
            y = jnp.dot(hid[e % 2], wd[e, :, cols], preferred_element_type=f32).astype(bf16).astype(f32)
            y = jnp.where(gate > 0.0, gate * y, 0.0)
            if e == 0:
                acc[:, cols] = y
            elif e < local - 1:
                acc[:, cols] += y
            else:
                ysend[pl.ds(base, pair), cols] = (acc[:, cols] + y).astype(bf16)

    def batch(b, carry):
        base = pl.multiple_of(b * pair, pair)
        for i in range(batches):
            @pl.when(b == i)
            def _(i=i):
                with scope('rwait%d' % i):
                    wait_rows(i)
        with scope('steps'):
            hidden(0, base)
            for e in range(1, local):
                hidden(e, base)
                down(e - 1, b, base)
            down(local - 1, b, base)
        for i in range(batches):
            @pl.when(b == i)
            def _(i=i):
                if i == own // 2:
                    yrecv[rows(own), :] = ysend[rows(own), :]
                for copies in zip(*[back_copies(k) for k in (2 * i + 1, 2 * i) if k != own]):
                    for copy in copies:
                        copy.start()
        return carry

    with scope('weights'):
        for copy in weights:
            copy.wait()
    lax.fori_loop(0, batches, batch, 0)

    def combine(i, cols):
        span = slice(i * pair, (i + 1) * pair)
        return lax.dot_general(pack[span, :], yrecv[span, cols], (((0,), (0,)), ((), ())), preferred_element_type=f32)

    everything = slice(0, d_model)
    wait_back(0, groups - 3, everything, 0)
    total[...] = x_ref[...].astype(f32) + combine(0, everything)
    for i in (1, batches - 1):
        total[...] += combine(i, everything)
    for h, cols in enumerate(halves):
        wait_back(2 * final, 2, cols, 1 + h)
        out_ref[:, cols] = (total[:, cols] + combine(final, cols)).astype(bf16)
    with scope('sends'):
        rank_copy.wait_send()
        remote(send.at[pl.ds(0, 6 * cap), :], recv.at[pl.ds(0, 6 * cap), :], row_send.at[0], row_recv.at[0], (0, 1)).wait_send()
        remote(sgate.at[pl.ds(0, groups - 1)], rgate.at[pl.ds(0, groups - 1)], gate_sem.at[0], gate_sem.at[1], (0, 1)).wait_send()
        remote(ysend.at[rows(0, groups - 1), :], yrecv.at[rows(0, groups - 1), :], back_send.at[0], back_recv.at[0], (0, 1)).wait_send()


def solution(mesh):
    groups = mesh.shape['ep']
    row_spec = P(('dp', 'ep'))
    expert_spec = P('ep')

    def device_step(tokens, expert_ids, gate_vals, w_gate, w_up, w_down):
        tok_dev, top_k = expert_ids.shape
        d_model = tokens.shape[1]
        local, _, ffn = w_gate.shape
        cap = tok_dev * (top_k // 2) // groups
        lanes = 128
        f32, bf16 = jnp.float32, jnp.bfloat16
        slots = groups * cap
        dma = pltpu.SemaphoreType.DMA
        return pl.pallas_call(
            functools.partial(moe_kernel, groups, cap),
            out_shape=pltpu.VMEM((tok_dev, d_model), bf16),
            in_specs=[pl.BlockSpec(memory_space=pl.ANY)] * 6,
            out_specs=pl.BlockSpec(memory_space=pltpu.VMEM),
            scratch_shapes=[
                pltpu.VMEM(tokens.shape, bf16),
                pltpu.VMEM((top_k, tok_dev), jnp.int32),
                pltpu.VMEM((top_k, tok_dev), f32),
                pltpu.VMEM(w_gate.shape, bf16),
                pltpu.VMEM(w_up.shape, bf16),
                pltpu.VMEM(w_down.shape, bf16),
                pltpu.VMEM((groups, tok_dev), f32),
                pltpu.VMEM((groups, tok_dev), jnp.int32),
                pltpu.VMEM((groups // 2, tok_dev), jnp.int32),
                pltpu.VMEM((groups // 2, tok_dev), jnp.int32),
                pltpu.VMEM(tokens.shape, bf16),
                pltpu.VMEM((slots // 2, tok_dev), bf16),
                pltpu.VMEM((slots, tok_dev), bf16),
                pltpu.VMEM((slots, d_model), bf16),
                pltpu.VMEM((groups, 4, lanes), f32),
                pltpu.VMEM((slots, d_model), bf16),
                pltpu.VMEM((groups + 1, 4, lanes), f32),
                pltpu.VMEM((groups // 2, 2 * cap, lanes), f32),
                pltpu.VMEM((2, 2 * cap, ffn), bf16),
                pltpu.VMEM((2 * cap, d_model), f32),
                pltpu.VMEM((slots, d_model), bf16),
                pltpu.VMEM((slots, d_model), bf16),
                pltpu.VMEM((tok_dev, d_model), f32),
                dma((3,)), dma((3,)), dma((1,)), dma((2,)), dma((2,)),
                dma((1,)), dma((groups // 2,)), dma((2,)), dma((1,)), dma((3,)), pltpu.SemaphoreType.REGULAR((3,)),
            ],
            compiler_params=pltpu.CompilerParams(collective_id=0, has_side_effects=True, vmem_limit_bytes=56 * 1024 * 1024),
        )(tokens, expert_ids.T, gate_vals.T, w_gate, w_up, w_down)

    return jax.shard_map(device_step, mesh=mesh, in_specs=(row_spec, row_spec, row_spec, expert_spec, expert_spec, expert_spec), out_specs=row_spec, check_vma=False)
```

```python
import contextlib
import functools

import jax
import jax.numpy as jnp
from jax import lax
from jax.experimental import pallas as pl
from jax.experimental.pallas import tpu as pltpu
from jax.sharding import PartitionSpec as P

MESH = pl.DeviceIdType.MESH
CORES = 2


def scope(name):
    return contextlib.nullcontext()


def moe_kernel(groups, cap, x_hbm, ids_hbm, gates_hbm, wg_hbm, wu_hbm, wd_hbm, out_ref,
               x_ref, ids_ref, gates_ref, wg, wu, wd, chosen, rank, nrank, rrank, raw, rpack, pack, send, sgate, recv, rgate,
               gcol, hid, acc, ysend, yrecv, total,
               in_sem, w_sem, raw_send, raw_recv, rank_sem, row_send, row_recv, gate_sem, back_send, back_recv, known):
    tok_dev, d_model = x_ref.shape
    local, _, ffn = wg.shape
    top_k = ids_ref.shape[0]
    lanes = sgate.shape[2]
    chips = groups // CORES
    batches = groups // 2
    pair = 2 * cap
    f32, bf16 = jnp.float32, jnp.bfloat16
    me = lax.axis_index('ep')
    chip, core = me // CORES, me % CORES
    side = 1 - 2 * core
    dests = [(side, 0), (side, 1), (-side, 0), (chips // 2, 0), (-side, 1), (chips // 2, 1), (0, 0), (0, 1)]
    homes = [(-side, 0), (side, 1), (side, 0), (chips // 2, 0), (-side, 1), (chips // 2, 1), (0, 0), (0, 1)]
    direct, near, own, partner = (2, 4), (1, 0, 3, 5), 6, 7
    relay_to = {1: (0, 1), 3: (side, 0), 5: (side, 1)}
    others = [k for k in range(groups) if k != own]

    def device(dx, dc):
        return lax.rem(chip + chips + dx, chips) * CORES + lax.rem(core + dc, CORES)

    def remote(src, dst, send_sem, recv_sem, to):
        return pltpu.make_async_remote_copy(
            src_ref=src, dst_ref=dst, send_sem=send_sem, recv_sem=recv_sem, device_id={'ep': device(*to)}, device_id_type=MESH)

    def rows(k, count=1):
        return pl.ds(k * cap, count * cap)

    def tell(sem, to):
        pl.semaphore_signal(sem, inc=1, device_id={'ep': device(*to)}, device_id_type=MESH)

    barrier = pltpu.get_barrier_semaphore()
    tell(barrier, (-side, 0))
    tell(barrier, (0, 1))

    inputs = [pltpu.make_async_copy(src, dst, in_sem.at[i])
              for i, (src, dst) in enumerate(((ids_hbm, ids_ref), (gates_hbm, gates_ref), (x_hbm, x_ref)))]
    weights = [pltpu.make_async_copy(src, dst, w_sem.at[i])
               for i, (src, dst) in enumerate(((wg_hbm, wg), (wu_hbm, wu), (wd_hbm, wd)))]

    early = d_model * 2 // 3
    halves = [slice(0, early), slice(early, d_model)]
    raw_copies = [remote(x_ref.at[:, cols], raw.at[:, cols], raw_send.at[0], raw_recv.at[h], (side, 0)) for h, cols in enumerate(halves)]
    rank_copy = remote(nrank, rrank, rank_sem.at[0], rank_sem.at[1], (side, 0))

    def row_copies(k):
        pieces = halves if k in relay_to else [slice(0, d_model)]
        return [remote(send.at[rows(k), cols], recv.at[rows(k), cols], row_send.at[0], row_recv.at[k // 2], relay_to.get(k, dests[k]))
                for cols in pieces]

    def gate_copy(k):
        return remote(sgate.at[k], rgate.at[k], gate_sem.at[0], gate_sem.at[1], dests[k])

    final = batches - 2
    ends = [slice(0, d_model - 2 * lanes), slice(d_model - 2 * lanes, d_model)]

    def back_copies(k):
        pieces = ends if k // 2 == final else [slice(0, d_model)]
        return [remote(ysend.at[rows(k), cols], yrecv.at[rows(k), cols], back_send.at[0], back_recv.at[0 if k // 2 != final else 1 + h], homes[k])
                for h, cols in enumerate(pieces)]

    def wait_rows(i):
        first, count = {0: (1, 1), batches - 1: (partner, 1)}.get(i, (2 * i, 2))
        remote(send.at[rows(first, count), :], recv.at[rows(first, count), :], row_send.at[0], row_recv.at[i], (0, 1)).wait_recv()

    def wait_back(first, count, cols, sem):
        remote(ysend.at[rows(first, count), cols], yrecv.at[rows(first, count), cols], back_send.at[0], back_recv.at[sem], (0, 1)).wait_recv()

    for copy in inputs:
        copy.start()
    inputs[2].wait()
    for copy in weights:
        copy.start()
    with scope('barrier'):
        pl.semaphore_wait(barrier, 2)
    tell(known.at[0], (side, 0))
    raw_copies[0].start()

    inputs[0].wait()
    inputs[1].wait()
    ids = ids_ref[...]
    gates = gates_ref[...]
    dev = ids // local
    for k in range(groups):
        chosen[k:k + 1, :] = jnp.max(jnp.where(dev == device(*dests[k]), 1.0, 0.0), axis=0, keepdims=True)
    flags = chosen[...]
    earlier = lax.broadcasted_iota(jnp.int32, (tok_dev, tok_dev), 0) < lax.broadcasted_iota(jnp.int32, (tok_dev, tok_dev), 1)
    order = jnp.dot(flags.astype(bf16), jnp.where(earlier, 1.0, 0.0).astype(bf16), preferred_element_type=f32)
    rank[...] = jnp.where(flags > 0.0, order, -1.0).astype(jnp.int32)
    for i, k in enumerate(near):
        nrank[i:i + 1, :] = rank[k:k + 1, :]
    rank_copy.start()
    with scope('known0'):
        pl.semaphore_wait(known.at[0], 1)
    tell(known.at[1], (-side, 0))

    row_id = lax.broadcasted_iota(jnp.int32, (lanes, tok_dev), 0)
    loc_id = lax.broadcasted_iota(jnp.int32, (local, tok_dev), 0)
    expert = lax.broadcasted_iota(jnp.int32, (local, lanes), 0).astype(f32)
    for k in (7, 2, 4, 6, 0, 1, 3, 5):
        onehot = jnp.where(row_id == rank[k:k + 1, :], 1.0, 0.0).astype(bf16)
        pack[rows(k), :] = onehot[:cap, :]
        first = device(*dests[k]) * local
        gate = jnp.zeros((local, tok_dev), f32)
        for j in range(top_k):
            gate += jnp.where(ids[j:j + 1, :] - first == loc_id, gates[j:j + 1, :], 0.0)
        high = jnp.minimum(gate, float(jnp.finfo(bf16).max)).astype(bf16).astype(f32)
        mid = (gate - high).astype(bf16).astype(f32)
        low = gate - high - mid
        parts = jnp.concatenate([high, mid, low], axis=0).astype(bf16)
        moved = lax.dot_general(parts, onehot, (((1,), (1,)), ((), ())), preferred_element_type=f32)
        moved = moved[:local] + moved[local:2 * local] + moved[2 * local:]
        low_id = jnp.min(jnp.where(moved > 0.0, expert, float(local)), axis=0, keepdims=True)
        high_id = jnp.max(jnp.where(moved > 0.0, expert, -1.0), axis=0, keepdims=True)
        moved = jnp.concatenate([jnp.sum(jnp.where(expert == low_id, moved, 0.0), axis=0, keepdims=True),
                                 jnp.sum(jnp.where(expert == high_id, moved, 0.0), axis=0, keepdims=True), low_id, high_id], axis=0)
        if k == own:
            rgate[groups] = moved
        else:
            sgate[k] = moved
    with scope('known1'):
        pl.semaphore_wait(known.at[1], 1)
    tell(known.at[2], (0, 1))
    with scope('known2'):
        pl.semaphore_wait(known.at[2], 1)
    for k in others:
        gate_copy(k).start()
    raw_copies[1].start()
    for k in (partner,) + direct + (own,):
        packed = jnp.dot(pack[rows(k), :], x_ref[...], preferred_element_type=f32).astype(bf16)
        if k == own:
            recv[rows(k), :] = packed
        else:
            send[rows(k), :] = packed
            if k == partner:
                for copy in row_copies(k):
                    copy.start()

    with scope('rankwait'):
        rank_copy.wait_recv()
    for i, k in enumerate(near):
        rpack[i * cap:(i + 1) * cap, :] = jnp.where(row_id[:cap, :] == rrank[i:i + 1, :], 1.0, 0.0).astype(bf16)

    def relay(i, h):
        k, cols = near[i], halves[h]
        packed = jnp.dot(rpack[i * cap:(i + 1) * cap, :], raw[:, cols], preferred_element_type=f32).astype(bf16)
        if k == 0:
            recv[rows(k), cols] = packed
        else:
            send[rows(k), cols] = packed

    with scope('raw0'):
        raw_copies[0].wait_recv()
    with scope('relay0'):
        for i in range(4):
            relay(i, 0)
        for k in (1, 3):
            row_copies(k)[0].start()
    with scope('gates'):
        remote(sgate.at[pl.ds(0, groups - 1)], rgate.at[pl.ds(0, groups - 1)], gate_sem.at[0], gate_sem.at[1], (0, 1)).wait_recv()
        for k in range(groups):
            two = rgate[groups if k == own else k]
            mine = jnp.where(expert == two[2:3], two[0:1], jnp.where(expert == two[3:4], two[1:2], 0.0))
            gcol[k // 2, (k % 2) * cap:(k % 2 + 1) * cap, :] = jnp.concatenate(
                [mine, jnp.zeros((lanes - local, lanes), f32)], axis=0).T[:cap, :]
    with scope('rawsend'):
        remote(x_ref, raw, raw_send.at[0], raw_recv.at[0], (side, 0)).wait_send()
    for k in direct:
        row_copies(k)[0].start()
    with scope('raw1'):
        raw_copies[1].wait_recv()
    with scope('relay1'):
        for i, k in enumerate(near):
            relay(i, 1)
            if k == 5:
                row_copies(k)[0].start()
            if k > 0:
                row_copies(k)[1].start()

    half = ffn // 2
    third = d_model // 3
    lane_id = lax.broadcasted_iota(jnp.int32, (pair, lanes), 1)

    def hidden(e, base):
        for n in range(2):
            cols = slice(n * half, (n + 1) * half)
            g = jnp.dot(recv[pl.ds(base, pair), :], wg[e, :, cols], preferred_element_type=f32)
            u = jnp.dot(recv[pl.ds(base, pair), :], wu[e, :, cols], preferred_element_type=f32)
            hid[e % 2, :, cols] = (jax.nn.silu(g) * u).astype(bf16)

    def down(e, b, base):
        gate = jnp.sum(jnp.where(lane_id == e, gcol[b], 0.0), axis=1, keepdims=True)
        for n in range(3):
            cols = slice(n * third, (n + 1) * third)
            y = jnp.dot(hid[e % 2], wd[e, :, cols], preferred_element_type=f32).astype(bf16).astype(f32)
            y = jnp.where(gate > 0.0, gate * y, 0.0)
            if e == 0:
                acc[:, cols] = y
            elif e < local - 1:
                acc[:, cols] += y
            else:
                ysend[pl.ds(base, pair), cols] = (acc[:, cols] + y).astype(bf16)

    def batch(b, carry):
        base = pl.multiple_of(b * pair, pair)
        for i in range(batches):
            @pl.when(b == i)
            def _(i=i):
                with scope('rwait%d' % i):
                    wait_rows(i)
        with scope('steps'):
            hidden(0, base)
            for e in range(1, local):
                hidden(e, base)
                down(e - 1, b, base)
            down(local - 1, b, base)
        for i in range(batches):
            @pl.when(b == i)
            def _(i=i):
                if i == own // 2:
                    yrecv[rows(own), :] = ysend[rows(own), :]
                for copies in zip(*[back_copies(k) for k in (2 * i + 1, 2 * i) if k != own]):
                    for copy in copies:
                        copy.start()
        return carry

    with scope('weights'):
        for copy in weights:
            copy.wait()
    lax.fori_loop(0, batches, batch, 0)

    def combine(i, cols):
        span = slice(i * pair, (i + 1) * pair)
        return lax.dot_general(pack[span, :], yrecv[span, cols], (((0,), (0,)), ((), ())), preferred_element_type=f32)

    everything = slice(0, d_model)
    wait_back(0, groups - 3, everything, 0)
    total[...] = x_ref[...].astype(f32) + combine(0, everything)
    for i in (1, batches - 1):
        total[...] += combine(i, everything)
    for h, cols in enumerate(ends):
        wait_back(2 * final, 2, cols, 1 + h)
        out_ref[:, cols] = (total[:, cols] + combine(final, cols)).astype(bf16)
    with scope('sends'):
        rank_copy.wait_send()
        remote(send.at[pl.ds(0, 6 * cap), :], recv.at[pl.ds(0, 6 * cap), :], row_send.at[0], row_recv.at[0], (0, 1)).wait_send()
        remote(sgate.at[pl.ds(0, groups - 1)], rgate.at[pl.ds(0, groups - 1)], gate_sem.at[0], gate_sem.at[1], (0, 1)).wait_send()
        remote(ysend.at[rows(0, groups - 1), :], yrecv.at[rows(0, groups - 1), :], back_send.at[0], back_recv.at[0], (0, 1)).wait_send()


def solution(mesh):
    groups = mesh.shape['ep']
    row_spec = P(('dp', 'ep'))
    expert_spec = P('ep')

    def device_step(tokens, expert_ids, gate_vals, w_gate, w_up, w_down):
        tok_dev, top_k = expert_ids.shape
        d_model = tokens.shape[1]
        local, _, ffn = w_gate.shape
        cap = tok_dev * (top_k // 2) // groups
        lanes = 128
        f32, bf16 = jnp.float32, jnp.bfloat16
        slots = groups * cap
        dma = pltpu.SemaphoreType.DMA
        return pl.pallas_call(
            functools.partial(moe_kernel, groups, cap),
            out_shape=pltpu.VMEM((tok_dev, d_model), bf16),
            in_specs=[pl.BlockSpec(memory_space=pl.ANY)] * 6,
            out_specs=pl.BlockSpec(memory_space=pltpu.VMEM),
            scratch_shapes=[
                pltpu.VMEM(tokens.shape, bf16),
                pltpu.VMEM((top_k, tok_dev), jnp.int32),
                pltpu.VMEM((top_k, tok_dev), f32),
                pltpu.VMEM(w_gate.shape, bf16),
                pltpu.VMEM(w_up.shape, bf16),
                pltpu.VMEM(w_down.shape, bf16),
                pltpu.VMEM((groups, tok_dev), f32),
                pltpu.VMEM((groups, tok_dev), jnp.int32),
                pltpu.VMEM((groups // 2, tok_dev), jnp.int32),
                pltpu.VMEM((groups // 2, tok_dev), jnp.int32),
                pltpu.VMEM(tokens.shape, bf16),
                pltpu.VMEM((slots // 2, tok_dev), bf16),
                pltpu.VMEM((slots, tok_dev), bf16),
                pltpu.VMEM((slots, d_model), bf16),
                pltpu.VMEM((groups, 4, lanes), f32),
                pltpu.VMEM((slots, d_model), bf16),
                pltpu.VMEM((groups + 1, 4, lanes), f32),
                pltpu.VMEM((groups // 2, 2 * cap, lanes), f32),
                pltpu.VMEM((2, 2 * cap, ffn), bf16),
                pltpu.VMEM((2 * cap, d_model), f32),
                pltpu.VMEM((slots, d_model), bf16),
                pltpu.VMEM((slots, d_model), bf16),
                pltpu.VMEM((tok_dev, d_model), f32),
                dma((3,)), dma((3,)), dma((1,)), dma((2,)), dma((2,)),
                dma((1,)), dma((groups // 2,)), dma((2,)), dma((1,)), dma((3,)), pltpu.SemaphoreType.REGULAR((3,)),
            ],
            compiler_params=pltpu.CompilerParams(collective_id=0, has_side_effects=True, vmem_limit_bytes=56 * 1024 * 1024),
        )(tokens, expert_ids.T, gate_vals.T, w_gate, w_up, w_down)

    return jax.shard_map(device_step, mesh=mesh, in_specs=(row_spec, row_spec, row_spec, expert_spec, expert_spec, expert_spec), out_specs=row_spec, check_vma=False)
```
